32 devices in a mesh: samp: 8 (over y, x, core), cpg: 4 (over z).
Axes of the slice: x: 2, y: 2, z: 4, core: 2. Of those that a mesh axis runs over, the one named last changes fastest.
Arguments:
- responses: bfloat16 [256, 16384], P('samp', 'cpg'), may hold values from -5 to 5
- weights: bfloat16 [256, 16384], P('samp', 'cpg'), may hold values from 1 to 8
- phenotype: float32 [16384], P('cpg'), may hold values from -6 to 6
- eigvecs: bfloat16 [16384, 16384], P('cpg', 'samp'), may hold values from -0.046875 to 0.046875
- eigvals: float32 [16384], P('samp'), may hold values from 0.0001 to 1
- positions: int32 [256], replicated, may hold values from 1 to 76800, as said below
- reaches: int32 [256], P('cpg'), may hold values from 1 to 8
Outputs:
- smoothed: float32 [256], P('cpg')
- log_scale: float32 [256], P('cpg')
The draws below stay inside these ranges and needn't reach their ends.
Inputs may be any that keep to these rules, and one draw needn't show every extreme that they name: CpG m (from 0) lies at 300 m plus an offset of 1 to 300, so positions strictly increase and consecutive CpGs lie 1 to 599 base pairs apart.
All inputs are finite; a program needn't handle non-finite values.
Results may differ from the reference program's by a relative error of at most 0.0041.
Values may be sent and summed in bfloat16 or wider, within the bound.
A program may use at most 64 MiB of HBM per device.

```python
import math
import jax
import jax.numpy as jnp
from jax import lax

N = 16384
ITERS = 4
HALO = 8
M = 256


def draw_positions(key, part):
    offsets = jax.random.randint(key, (M,), 1, 301)
    index = jnp.arange(M, dtype=jnp.int32)
    offsets = jnp.where(index == 0, 1, offsets)
    offsets = jnp.where(index == M - 1, 300, offsets)
    return (300 * index + offsets).astype(jnp.int32)


def draw_working(key):
    root_key = jax.random.fold_in(key, 4049)
    weight_key = jax.random.fold_in(root_key, 1)
    noise_key = jax.random.fold_in(root_key, 2)
    excess_key = jax.random.fold_in(root_key, 3)
    weight_draw = jnp.exp(jax.random.uniform(weight_key, (M, N), jnp.float32, 0.0, jnp.log(8.0)))
    noise_draw = jnp.clip(jax.random.normal(noise_key, (M, N), jnp.float32), -4.0, 4.0)
    weight_draw = jnp.clip(weight_draw, 1.0, 8.0).astype(jnp.bfloat16)
    excess = 0.04 * jnp.exp(jax.random.uniform(excess_key, (M, 1), jnp.float32, 0.0, jnp.log(5.0)))
    row_scale = jnp.sqrt((1.0 + excess) / weight_draw.astype(jnp.float32))
    response_draw = jnp.clip(row_scale * noise_draw, -5.0, 5.0).astype(jnp.bfloat16)
    return (weight_draw, response_draw)


def draw_weights(key, part):
    return draw_working(key)[0]


def draw_responses(key, part):
    return draw_working(key)[1]


def plant(array, stream_key, smallest, top_value):
    spot = [jax.random.randint(jax.random.fold_in(stream_key, axis), (), 0, length) for axis, length in enumerate(array.shape)]
    widest = array.shape.index(max(array.shape))
    neighbour = spot[:widest] + [(spot[widest] + 1) % array.shape[widest]] + spot[widest + 1:]
    return array.at[tuple(spot)].set(smallest).at[tuple(neighbour)].set(top_value)


def steps_of(key, extent, split, low, high):
    factor_of = 1.0
    for axis_at, blocks in split:
        draws = jax.random.uniform(jax.random.fold_in(jax.random.fold_in(key, 6), axis_at), (blocks,), jnp.float32, low / len(split), high / len(split))
        factor_of = factor_of * jnp.repeat(jnp.exp(draws), extent[axis_at] // blocks).reshape((-1,) + (1,) * (len(extent) - 1 - axis_at))
    return factor_of


def noise(stream_key, shape, scale, most, shards=(), kind=jnp.bfloat16):
    array = scale * jax.random.normal(stream_key, shape, jnp.float32)
    if shards:
        array = array * steps_of(stream_key, shape, shards, -0.22, 0.18)
    return jnp.clip(array, -most, most).astype(kind)


def setup_inputs(seed: int = 0) -> dict:
    key_of = jax.random.split(jax.random.key(seed), 8)
    return {
        "responses": draw_responses(jax.random.fold_in(key_of[7], 71), 0),
        "weights": draw_weights(jax.random.fold_in(key_of[7], 71), 0),
        "phenotype": noise(key_of[2], (N,), 1.0, 6.0, ((0, 4),), jnp.float32),
        "eigvecs": noise(key_of[3], (N, N), N ** -0.5, 0.046875, ((0, 4), (1, 8))),
        "eigvals": jnp.clip(jnp.exp(math.log(1.0) - 9.2103404 * jax.random.uniform(key_of[4], (N,), jnp.float32) ** steps_of(key_of[4], (N,), ((0, 8),), -0.2, 0.2)), 0.0001, 1.0),
        "positions": draw_positions(jax.random.fold_in(key_of[7], 71), 0),
        "reaches": plant(jax.random.randint(key_of[6], (M,), 1, HALO + 1), jax.random.fold_in(key_of[6], 1), 1, HALO).astype(jnp.int32),
    }


EPSILON = 1e-06
band_width = 1000.0

def smooth_block(widened, places, present, reaches):
    block_len = reaches.shape[0]
    centre = places[HALO:HALO + block_len]
    total_sum = jnp.zeros((block_len,), jnp.float32)
    norm_sum = jnp.zeros((block_len,), jnp.float32)
    for offset in range(2 * HALO + 1):
        near_scores = widened[offset:offset + block_len]
        near_places = places[offset:offset + block_len]
        within = (abs(offset - HALO) <= reaches).astype(jnp.float32)
        kernel = present[offset:offset + block_len] * within * jnp.exp(-jnp.abs(near_places - centre) / band_width)
        total_sum = total_sum + kernel * near_scores
        norm_sum = norm_sum + kernel
    return total_sum / norm_sum

def reference(responses, weights, phenotype, eigvecs, eigvals, positions, reaches):
    root_weight = jnp.sqrt(weights.astype(jnp.float32))
    weighted = (root_weight * responses.astype(jnp.float32)).astype(jnp.bfloat16)
    design = (root_weight * phenotype[None, :]).astype(jnp.bfloat16)
    rot_resp = jnp.dot(weighted, eigvecs, preferred_element_type=jnp.float32)
    rot_design = jnp.dot(design, eigvecs, preferred_element_type=jnp.float32)
    eigen_part = eigvals[None, :]
    log_scale = jnp.zeros((M,), jnp.float32)
    for repeat in range(ITERS):
        inverse = 1.0 / (jnp.exp(log_scale)[:, None] * eigen_part + 1.0)
        crossed = lax.optimization_barrier(jnp.sum(rot_design * rot_resp * inverse, axis=1))
        energy = lax.optimization_barrier(jnp.sum(rot_design * rot_design * inverse, axis=1)) + EPSILON
        effect = crossed / energy
        residual = rot_resp - effect[:, None] * rot_design
        spread = lax.optimization_barrier(jnp.sum(eigen_part * residual * residual * inverse * inverse, axis=1))
        traced = lax.optimization_barrier(jnp.sum(eigen_part * inverse, axis=1))
        fisher = 0.5 * lax.optimization_barrier(jnp.sum(eigen_part * eigen_part * inverse * inverse, axis=1))
        gradient = 0.5 * (spread - traced)
        log_scale = log_scale + jnp.tanh(gradient / (jnp.exp(log_scale) * fisher))
    inverse = 1.0 / (jnp.exp(log_scale)[:, None] * eigen_part + 1.0)
    crossed = lax.optimization_barrier(jnp.sum(rot_design * rot_resp * inverse, axis=1))
    energy = lax.optimization_barrier(jnp.sum(rot_design * rot_design * inverse, axis=1)) + EPSILON
    zscore = crossed / jnp.sqrt(energy)
    widened = jnp.pad(zscore, HALO)
    places = jnp.pad(positions.astype(jnp.float32), HALO)
    present = jnp.pad(jnp.ones((M,), jnp.float32), HALO)
    smoothed = smooth_block(widened, places, present, reaches)
    return (smoothed, log_scale)
```

```python
import functools

import jax
import jax.numpy as jnp
from jax import lax
from jax.experimental import pallas as pl
from jax.experimental.pallas import tpu as pltpu
from jax.sharding import PartitionSpec as P

ITERS = 4
HALO = 8
EPSILON = 1e-06
band_width = 1000.0
MESH = pl.DeviceIdType.MESH
LANES = 128
CHUNK = 256
SKEW = 4
STRIP = 512


def score_kernel(n, cpgs, w_hbm, r_hbm, ph_ref, v_hbm, lam_ref, pos_ref, reach_ref, out_ref,
                 wbuf, rbuf, g, v, part, sent, landed, full, pp, qq, rr, lb, lamg, mail, got, pad, band,
                 wsem, vsem, gs, gr, ls, lr, zs, zr, hs, hr, es, er, bs, br):
    me = lax.axis_index("samp")
    mz = lax.axis_index("cpg")
    last = cpgs - 1
    each, samples = wbuf.shape
    half = each // 2
    pair = 2 * half
    side = 2 * pair
    phases = g.shape[0]
    chunks = v.shape[0]
    units = phases * chunks
    total = each * n
    block = total // cpgs
    bits = [1 << i for i in range(1, n.bit_length() - 1)]
    orders = (bits, bits[::-1])
    pieces = gs.shape[2]
    cols = samples // pieces
    is_end = (mz == 0) | (mz == last)

    def mask_of(h, j):
        return sum(bit for i, bit in enumerate(orders[h]) if (j >> i) & 1)

    def flipped(mask):
        out = me
        bit = 1
        while bit <= mask:
            if mask & bit:
                out = out + bit - 2 * bit * lax.rem(lax.div(me, bit), 2)
            bit *= 2
        return out

    loads = [pltpu.make_async_copy(w_hbm, wbuf, wsem.at[0]), pltpu.make_async_copy(r_hbm, rbuf, wsem.at[1])]
    for c in loads:
        c.start()

    def load(c):
        return pltpu.make_async_copy(v_hbm.at[:, pl.ds(pl.multiple_of(c * CHUNK, CHUNK), CHUNK)], v.at[c], vsem.at[c])

    for c in range(chunks):
        load(c).start()

    got[...] = jnp.zeros_like(got)
    barrier = pltpu.get_barrier_semaphore()
    for j in range(1, n):
        pl.semaphore_signal(barrier, inc=1, device_id={"samp": flipped(j)}, device_id_type=MESH)

    @pl.when(mz > 0)
    def _():
        pl.semaphore_signal(barrier, inc=1, device_id={"cpg": lax.max(mz - 1, 0)}, device_id_type=MESH)

    @pl.when(mz < last)
    def _():
        pl.semaphore_signal(barrier, inc=1, device_id={"cpg": lax.min(mz + 1, last)}, device_id_type=MESH)

    for c in loads:
        c.wait()

    def rows_of(h, cb):
        return pl.ds(h * side + cb * pair, pair)

    def prepare(i, carry):
        at = pl.ds(pl.multiple_of(i * STRIP, STRIP), STRIP)
        root = jnp.sqrt(wbuf[:, at].astype(jnp.float32))
        weighted = (root * rbuf[:, at].astype(jnp.float32)).astype(jnp.bfloat16)
        design = (root * ph_ref[:, at]).astype(jnp.bfloat16)
        for h in range(2):
            g[0, pl.ds(h * side, half), at] = weighted[h * half : (h + 1) * half]
            g[0, pl.ds(h * side + half, half), at] = design[h * half : (h + 1) * half]
        return carry

    lax.fori_loop(0, samples // STRIP, prepare, 0)

    def piece(q):
        return pl.ds(pl.multiple_of(q * cols, cols), cols)

    def ship(h, src, dst, q, bit):
        return pltpu.make_async_remote_copy(
            src_ref=g.at[src, rows_of(h, 0), piece(q)], dst_ref=g.at[dst, rows_of(h, 0), piece(q)],
            send_sem=gs.at[h, dst, q], recv_sem=gr.at[h, dst, q],
            device_id={"samp": flipped(bit)}, device_id_type=MESH)

    def share(h, j, q):
        return pltpu.make_async_remote_copy(
            src_ref=g.at[j, rows_of(h, 0), piece(q)], dst_ref=g.at[j, rows_of(h, 1), piece(q)],
            send_sem=ls.at[h, j, q], recv_sem=lr.at[h, j, q],
            device_id={"samp": flipped(1)}, device_id_type=MESH)

    pl.semaphore_wait(barrier, n - 1 + (mz > 0).astype(jnp.int32) + (mz < last).astype(jnp.int32))

    for q in range(pieces):
        for h in range(2):
            ship(h, 0, 1, q, orders[h][0]).start()
    for q in range(pieces):
        for h in range(2):
            share(h, 0, q).start()
    for i in range(1, len(bits)):
        for q in range(pieces):
            for h in range(2):
                ship(h, 0, 1 << i, q, orders[h][i]).start()

    lane = lax.broadcasted_iota(jnp.int32, (8, LANES), 1)

    def spread_out(cur, before, after):
        right = pltpu.roll(after, block, 1)
        left = pltpu.roll(before, LANES - block, 1)
        return jnp.where(lane < block, cur, jnp.where(lane < block + HALO, right, left))

    def spots(b):
        at = b * block
        row = pos_ref[0:1, pl.ds(pl.multiple_of(lax.div(at, LANES) * LANES, LANES), LANES)].astype(jnp.float32)
        return pltpu.roll(jnp.broadcast_to(row, (8, LANES)), lax.rem(LANES - lax.rem(at, LANES), LANES), 1)

    pad[...] = jnp.zeros_like(pad)
    pad[0:1, 0:block] = reach_ref[...]
    reach = jnp.broadcast_to(pad[0:1, :], (8, LANES))
    places = spread_out(spots(mz), spots(lax.max(mz - 1, 0)), spots(lax.min(mz + 1, last)))
    norm = jnp.zeros((8, LANES), jnp.float32)
    for o in range(2 * HALO + 1):
        shift = (HALO - o) % LANES
        near = pltpu.roll(places, shift, 1) if shift else places
        at = mz * block + lane + (o - HALO)
        keep = (at >= 0) & (at < total) & (abs(o - HALO) <= reach)
        c = jnp.where(keep, jnp.exp(-jnp.abs(near - places) / band_width), 0.0)
        band[o] = c
        norm = norm + c
    band[2 * HALO + 1] = jnp.where(lane < block, norm, 1.0)
    lamg[0] = lam_ref[...]

    def greet(mask):
        return pltpu.make_async_remote_copy(
            src_ref=lam_ref, dst_ref=lamg.at[mask], send_sem=es.at[mask], recv_sem=er.at[mask],
            device_id={"samp": flipped(mask)}, device_id_type=MESH)

    def chain(d, i):
        return pltpu.make_async_remote_copy(
            src_ref=sent.at[d, i], dst_ref=landed.at[d, i], send_sem=zs.at[d, i], recv_sem=zr.at[d, i],
            device_id={"cpg": lax.min(mz + 1, last) if d else lax.max(mz - 1, 0)}, device_id_type=MESH)

    def hand(d, j, c, cb):
        slot = mask_of(d, j) | cb
        return pltpu.make_async_remote_copy(
            src_ref=sent.at[d, j * chunks + c, pl.ds(cb * pair, pair)], dst_ref=full.at[slot, c],
            send_sem=hs.at[j * chunks + c, cb], recv_sem=hr.at[slot, c],
            device_id={"samp": flipped(slot)}, device_id_type=MESH)

    def deliver(d, i):
        for j in range(phases):
            @pl.when(lax.div(i, chunks) == j)
            def _():
                c = i - j * chunks
                if j == 0:
                    full[0, c] = sent[d, i, 0:pair, :]
                    hand(d, 0, c, 1).start()
                elif j == phases - 1:
                    for cb in range(2):
                        hand(d, j, c, cb).start()
                elif j == phases - 2:
                    for held in range(1, phases - 1):
                        for cb in range(2):
                            hand(d, held, c, cb).start()

    def advance(d, i, first, end):
        own = part[i, pl.ds(d * side, side), :]

        @pl.when(first)
        def _():
            sent[d, i] = own.astype(jnp.bfloat16)

        @pl.when(jnp.logical_not(first))
        def _():
            chain(d, i).wait_recv()
            sent[d, i] = (own + landed[d, i].astype(jnp.float32)).astype(jnp.bfloat16)

        @pl.when(jnp.logical_not(end))
        def _():
            chain(d, i).start()

        @pl.when(end)
        def _():
            deliver(d, i)

    def turn(t, carry):
        j = lax.div(t, chunks)
        c = t - j * chunks

        @pl.when(t < chunks)
        def _():
            load(c).wait()

        @pl.when((c == 0) & (t < units))
        def _():
            for q in range(pieces):
                for h in range(2):
                    share(h, j, q).wait_recv()

        @pl.when((t == (phases - 1) * chunks) & is_end)
        def _():
            for mask in range(1, n):
                greet(mask).start()

        @pl.when(t < units)
        def _():
            part[t] = jnp.dot(g[j], v[c], preferred_element_type=jnp.float32)

        up = t - SKEW * mz

        @pl.when((up >= 0) & (up < units))
        def _():
            advance(1, up, mz == 0, mz == last)

        down = t - SKEW * (last - mz)

        @pl.when((down >= 0) & (down < units))
        def _():
            advance(0, down, mz == last, mz == 0)

        q = lax.div(c, 2)
        for nxt in range(1, phases):
            for h in range(2):
                @pl.when((j == nxt - 1) & (lax.rem(c, 2) == h))
                def _():
                    top = nxt.bit_length() - 1
                    ship(h, nxt - (1 << top), nxt, q, orders[h][top]).wait_recv()
                    share(h, nxt, q).start()
                    for i in range(top + 1, len(bits)):
                        ship(h, nxt, nxt | (1 << i), q, orders[h][i]).start()

        return carry

    lax.fori_loop(0, units + SKEW * last, turn, 0)

    row = lax.broadcasted_iota(jnp.int32, (half, LANES), 0)
    lane_of = lax.broadcasted_iota(jnp.int32, (half, LANES), 1)
    which = (mz == last).astype(jnp.int32)
    base = me * each + which * half
    home = lax.div(base, block)
    slot_mine = which * n + me

    def post(step, i):
        return pltpu.make_async_remote_copy(
            src_ref=mail, dst_ref=got.at[slot_mine], send_sem=bs.at[step, i], recv_sem=br.at[slot_mine],
            device_id={"samp": lax.rem(me + i, n), "cpg": lax.clamp(0, home + step - 1, last)}, device_id_type=MESH)

    def each_post(act):
        for step in range(3):
            plane = home + step - 1

            @pl.when((plane >= 0) & (plane <= last))
            def _():
                def body(i, carry):
                    @pl.when((i > 0) | (plane != mz))
                    def _():
                        act(post(step, i))
                    return carry

                lax.fori_loop(0, n, body, 0)

    def fold(x):
        return sum(x[:, k * LANES : (k + 1) * LANES] for k in range(CHUNK // LANES))

    def tall(x):
        return jnp.concatenate([x] * (half // 8), axis=0)

    def settle(acc):
        return [jnp.sum(x, axis=1, keepdims=True) for x in acc]

    def newton(log_scale, acc):
        crossed, energy, traced, fisher, s_r, s_p, s_q = settle(acc)
        effect = crossed / (energy + EPSILON)
        spread = s_r - 2.0 * effect * s_p + effect * effect * s_q
        gradient = 0.5 * (spread - traced)
        return log_scale + jnp.tanh(gradient / (jnp.exp(log_scale) * (0.5 * fisher)))

    @pl.when(is_end)
    def _():
        acc = tuple(jnp.zeros((half if k < 5 else 8, LANES), jnp.float32) for k in range(7))
        for j in range(phases):
            for cb in range(2):
                here = j == 0 and cb == 0
                slot = jnp.where(mz == 0, mask_of(0, j) + cb, mask_of(1, j) + cb)

                if not here:
                    pltpu.make_async_remote_copy(
                        src_ref=lam_ref, dst_ref=lamg.at[slot], send_sem=es.at[slot], recv_sem=er.at[slot],
                        device_id={"samp": flipped(1)}, device_id_type=MESH).wait_recv()

                def absorb(c, acc):
                    if not here:
                        pltpu.make_async_remote_copy(
                            src_ref=sent.at[0, 0, pl.ds(0, pair)], dst_ref=full.at[slot, c],
                            send_sem=hs.at[0, 0], recv_sem=hr.at[slot, c],
                            device_id={"samp": flipped(1)}, device_id_type=MESH).wait_recv()
                    at = slot * chunks + c
                    a = full[slot, c, 0:half, :].astype(jnp.float32)
                    b = full[slot, c, half:pair, :].astype(jnp.float32)
                    p, q, r = a * b, b * b, a * a
                    pp[at] = p
                    qq[at] = q
                    rr[at] = r
                    lam = lamg[slot, 0:1, pl.ds(pl.multiple_of(c * CHUNK, CHUNK), CHUNK)]
                    lam = jnp.broadcast_to(lam, (8, CHUNK))
                    lb[at] = lam
                    inv = 1.0 / (lam + 1.0)
                    lev = lam * inv
                    s = tall(lev * inv)
                    inv = tall(inv)
                    terms = (p * inv, q * inv, s * r, s * p, s * q, lev, lev * lev)
                    return tuple(x + fold(y) for x, y in zip(acc, terms))

                acc = lax.fori_loop(0, chunks, absorb, acc)
        crossed, energy, s_r, s_p, s_q, traced, fisher = acc
        log_scale = newton(jnp.zeros((half, 1), jnp.float32),
                           (crossed, energy, tall(traced), tall(fisher), s_r, s_p, s_q))

        def sweep(log_scale, whole):
            scale = jnp.broadcast_to(jnp.exp(log_scale), (half, CHUNK))

            def body(i, acc):
                lam = tall(lb[i])
                inv = 1.0 / (scale * lam + 1.0)
                p = pp[i]
                q = qq[i]
                terms = [p * inv, q * inv]
                if whole:
                    lev = lam * inv
                    s = lev * inv
                    terms += [lev, lev * lev, s * rr[i], s * p, s * q]
                return tuple(x + fold(y) for x, y in zip(acc, terms))

            start = tuple(jnp.zeros((half, LANES), jnp.float32) for _ in range(7 if whole else 2))
            return lax.fori_loop(0, n * chunks, body, start)

        for _ in range(ITERS - 1):
            log_scale = newton(log_scale, sweep(log_scale, True))
        crossed, energy = settle(sweep(log_scale, False))
        zscore = crossed / jnp.sqrt(energy + EPSILON)
        hit = lane_of == row + lax.rem(base, block)
        mail[0:1, :] = jnp.sum(jnp.where(hit, jnp.broadcast_to(zscore, (half, LANES)), 0.0), axis=0, keepdims=True)
        mail[1:2, :] = jnp.sum(jnp.where(hit, jnp.broadcast_to(log_scale, (half, LANES)), 0.0), axis=0, keepdims=True)
        each_post(lambda copy: copy.start())

        @pl.when((home >= mz - 1) & (home <= mz + 1))
        def _():
            got[slot_mine] = mail[...]

    cur = jnp.zeros((2, LANES), jnp.float32)
    before = cur
    after = cur
    for h in range(2):
        for s in range(n):
            spot = (s * each + h * half) // block
            mine = (me == s) & (mz == (last if h else 0))

            @pl.when((mz >= spot - 1) & (mz <= spot + 1) & jnp.logical_not(mine))
            def _():
                pltpu.make_async_remote_copy(
                    src_ref=mail, dst_ref=got.at[h * n + s], send_sem=bs.at[0, 0], recv_sem=br.at[h * n + s],
                    device_id={"samp": flipped(1)}, device_id_type=MESH).wait_recv()

    for h in range(2):
        for s in range(n):
            spot = (s * each + h * half) // block
            value = got[h * n + s]
            cur = cur + jnp.where(mz == spot, value, 0.0)
            before = before + jnp.where(mz - 1 == spot, value, 0.0)
            after = after + jnp.where(mz + 1 == spot, value, 0.0)

    def tile(x, k):
        return jnp.broadcast_to(x[k : k + 1, :], (8, LANES))

    wide = spread_out(tile(cur, 0), tile(before, 0), tile(after, 0))
    acc = jnp.zeros((8, LANES), jnp.float32)
    for o in range(2 * HALO + 1):
        shift = (HALO - o) % LANES
        near = pltpu.roll(wide, shift, 1) if shift else wide
        acc = acc + band[o] * near
    top = lax.broadcasted_iota(jnp.int32, (8, LANES), 0)
    out_ref[...] = jnp.where(top == 0, acc / band[2 * HALO + 1], tile(cur, 1))

    def drain_gather(i, carry):
        for h in range(2):
            for j in range(phases):
                share(h, j, i).wait_send()
                if j:
                    bit = j.bit_length() - 1
                    ship(h, j - (1 << bit), j, i, orders[h][bit]).wait_send()
        return carry

    lax.fori_loop(0, pieces, drain_gather, 0)

    def drain_chain(i, carry):
        @pl.when(mz < last)
        def _():
            chain(1, i).wait_send()

        @pl.when(mz > 0)
        def _():
            chain(0, i).wait_send()
        return carry

    lax.fori_loop(0, units, drain_chain, 0)

    @pl.when(is_end)
    def _():
        for mask in range(1, n):
            greet(mask).wait_send()
        each_post(lambda copy: copy.wait_send())

        def drain_hand(c, carry):
            for j in range(phases):
                for cb in range(2):
                    if j or cb:
                        hand(0, j, c, cb).wait_send()
            return carry

        lax.fori_loop(0, chunks, drain_hand, 0)


def scores(weights, responses, phenotype, eigvecs, eigvals, positions, reaches, n, cpgs):
    each, samples = weights.shape
    comps = eigvecs.shape[1]
    chunks = comps // CHUNK
    phases = n // 2
    units = phases * chunks
    half = each // 2
    pair = 2 * half
    side = 2 * pair
    total = each * n
    pieces = max(chunks // 2, 1)
    vmem = pl.BlockSpec(memory_space=pltpu.VMEM)
    hbm = pl.BlockSpec(memory_space=pl.ANY)
    dma = pltpu.SemaphoreType.DMA
    travel = pltpu.VMEM((2, units, side, CHUNK), jnp.bfloat16)
    big = pltpu.VMEM((n * chunks, half, CHUNK), jnp.float32)
    return pl.pallas_call(
        functools.partial(score_kernel, n, cpgs),
        out_shape=jax.ShapeDtypeStruct((8, LANES), jnp.float32),
        in_specs=[hbm, hbm, vmem, hbm, vmem, vmem, vmem],
        out_specs=vmem,
        scratch_shapes=[
            pltpu.VMEM((each, samples), jnp.bfloat16),
            pltpu.VMEM((each, samples), jnp.bfloat16),
            pltpu.VMEM((phases, 2 * side, samples), jnp.bfloat16),
            pltpu.VMEM((chunks, samples, CHUNK), jnp.bfloat16),
            pltpu.VMEM((units, 2 * side, CHUNK), jnp.float32),
            travel, travel,
            pltpu.VMEM((n, chunks, pair, CHUNK), jnp.bfloat16),
            big, big, big,
            pltpu.VMEM((n * chunks, 8, CHUNK), jnp.float32),
            pltpu.VMEM((n, 1, comps), jnp.float32),
            pltpu.VMEM((2, LANES), jnp.float32),
            pltpu.VMEM((2 * n, 2, LANES), jnp.float32),
            pltpu.VMEM((8, LANES), jnp.int32),
            pltpu.VMEM((2 * HALO + 2, 8, LANES), jnp.float32),
            dma((2,)), dma((chunks,)),
            dma((2, phases, pieces)), dma((2, phases, pieces)),
            dma((2, phases, pieces)), dma((2, phases, pieces)),
            dma((2, units)), dma((2, units)),
            dma((units, 2)), dma((n, chunks)),
            dma((n,)), dma((n,)),
            dma((3, n)), dma((2 * n,)),
        ],
        compiler_params=pltpu.CompilerParams(collective_id=1, has_side_effects=True, vmem_limit_bytes=60 * 1024 * 1024),
        cost_estimate=pl.CostEstimate(flops=4 * total * samples * comps, bytes_accessed=2 * samples * comps, transcendentals=0),
        name="scores",
    )(weights, responses, phenotype[None, :], eigvecs, eigvals[None, :], positions[None, :], reaches[None, :])


def shards(responses, weights, phenotype, eigvecs, eigvals, positions, reaches):
    n, cpgs = lax.axis_size("samp"), lax.axis_size("cpg")
    out = scores(weights, responses, phenotype, eigvecs, eigvals, positions, reaches, n, cpgs)
    block = reaches.shape[0]
    return (out[0, :block], out[1, :block])


def solution(mesh):
    in_specs = (P("samp", "cpg"), P("samp", "cpg"), P("cpg"), P("cpg", "samp"), P("samp"), P(), P("cpg"))
    out_specs = (P("cpg"), P("cpg"))
    return jax.shard_map(shards, mesh=mesh, in_specs=in_specs, out_specs=out_specs, check_vma=False)
```

```python
import functools

import jax
import jax.numpy as jnp
from jax import lax
from jax.experimental import pallas as pl
from jax.experimental.pallas import tpu as pltpu
from jax.sharding import PartitionSpec as P

ITERS = 4
HALO = 8
EPSILON = 1e-06
band_width = 1000.0
MESH = pl.DeviceIdType.MESH
LANES = 128
CHUNK = 256
SKEW = 4
STRIP = 512
AHEAD = 3
UNROLL = 4


def score_kernel(n, cpgs, w_hbm, r_hbm, ph_ref, v_hbm, lam_ref, pos_ref, reach_ref, out_ref,
                 wbuf, rbuf, g, v, part, sent, landed, full, pp, qq, rr, lb, lamg, mail, got, pad, band,
                 wsem, vsem, gs, gr, ls, lr, zs, zr, hs, hr, es, er, bs, br):
    me = lax.axis_index("samp")
    mz = lax.axis_index("cpg")
    last = cpgs - 1
    each, samples = wbuf.shape
    half = each // 2
    pair = 2 * half
    side = 2 * pair
    phases = g.shape[0]
    chunks = v.shape[0]
    units = phases * chunks
    total = each * n
    block = total // cpgs
    bits = [1 << i for i in range(1, n.bit_length() - 1)]
    orders = (bits, bits[::-1])
    pieces = gr.shape[2]
    cols = samples // pieces
    is_end = (mz == 0) | (mz == last)

    def mask_of(h, j):
        return sum(bit for i, bit in enumerate(orders[h]) if (j >> i) & 1)

    def flipped(mask):
        out = me
        bit = 1
        while bit <= mask:
            if mask & bit:
                out = out + bit - 2 * bit * lax.rem(lax.div(me, bit), 2)
            bit *= 2
        return out

    loads = [pltpu.make_async_copy(w_hbm, wbuf, wsem.at[0]), pltpu.make_async_copy(r_hbm, rbuf, wsem.at[1])]
    for c in loads:
        c.start()

    def load(c):
        return pltpu.make_async_copy(v_hbm.at[:, pl.ds(pl.multiple_of(c * CHUNK, CHUNK), CHUNK)], v.at[c], vsem.at[c])

    got[...] = jnp.zeros_like(got)
    barrier = pltpu.get_barrier_semaphore()
    for j in range(1, n):
        pl.semaphore_signal(barrier, inc=1, device_id={"samp": flipped(j)}, device_id_type=MESH)

    @pl.when(mz > 0)
    def _():
        pl.semaphore_signal(barrier, inc=1, device_id={"cpg": lax.max(mz - 1, 0)}, device_id_type=MESH)

    @pl.when(mz < last)
    def _():
        pl.semaphore_signal(barrier, inc=1, device_id={"cpg": lax.min(mz + 1, last)}, device_id_type=MESH)

    with jax.named_scope("loadwait"):
        for c in loads:
            c.wait()
    for c in range(min(AHEAD, chunks)):
        load(c).start()

    def rows_of(h, cb):
        return pl.ds(h * side + cb * pair, pair)

    def prepare(i, carry):
        at = pl.ds(pl.multiple_of(i * STRIP, STRIP), STRIP)
        root = jnp.sqrt(wbuf[:, at].astype(jnp.float32))
        weighted = (root * rbuf[:, at].astype(jnp.float32)).astype(jnp.bfloat16)
        design = (root * ph_ref[:, at]).astype(jnp.bfloat16)
        for h in range(2):
            g[0, pl.ds(h * side, half), at] = weighted[h * half : (h + 1) * half]
            g[0, pl.ds(h * side + half, half), at] = design[h * half : (h + 1) * half]
        return carry

    with jax.named_scope("prep"):
        lax.fori_loop(0, samples // STRIP, prepare, 0)

    def piece(q):
        return pl.ds(pl.multiple_of(q * cols, cols), cols)

    def ship(h, src, dst, q, bit):
        return pltpu.make_async_remote_copy(
            src_ref=g.at[src, rows_of(h, 0), piece(q)], dst_ref=g.at[dst, rows_of(h, 0), piece(q)],
            send_sem=gs.at[h], recv_sem=gr.at[h, dst, q],
            device_id={"samp": flipped(bit)}, device_id_type=MESH)

    def share(h, j, q):
        return pltpu.make_async_remote_copy(
            src_ref=g.at[j, rows_of(h, 0), piece(q)], dst_ref=g.at[j, rows_of(h, 1), piece(q)],
            send_sem=ls.at[h], recv_sem=lr.at[h, j],
            device_id={"samp": flipped(1)}, device_id_type=MESH)

    pl.semaphore_wait(barrier, n - 1 + (mz > 0).astype(jnp.int32) + (mz < last).astype(jnp.int32))

    for q in range(pieces):
        for h in range(2):
            ship(h, 0, 1, q, orders[h][0]).start()
    for q in range(pieces):
        for h in range(2):
            share(h, 0, q).start()

    def shared(h, j):
        return pltpu.make_async_remote_copy(
            src_ref=g.at[j, rows_of(h, 0)], dst_ref=g.at[j, rows_of(h, 1)], send_sem=ls.at[h], recv_sem=lr.at[h, j],
            device_id={"samp": flipped(1)}, device_id_type=MESH)

    def top_of(j):
        return j.bit_length() - 1

    lane = lax.broadcasted_iota(jnp.int32, (8, LANES), 1)

    def spread_out(cur, before, after):
        right = pltpu.roll(after, block, 1)
        left = pltpu.roll(before, LANES - block, 1)
        return jnp.where(lane < block, cur, jnp.where(lane < block + HALO, right, left))

    def spots(b):
        at = b * block
        row = pos_ref[0:1, pl.ds(pl.multiple_of(lax.div(at, LANES) * LANES, LANES), LANES)].astype(jnp.float32)
        return pltpu.roll(jnp.broadcast_to(row, (8, LANES)), lax.rem(LANES - lax.rem(at, LANES), LANES), 1)

    pad[...] = jnp.zeros_like(pad)
    pad[0:1, 0:block] = reach_ref[...]
    reach = jnp.broadcast_to(pad[0:1, :], (8, LANES))
    places = spread_out(spots(mz), spots(lax.max(mz - 1, 0)), spots(lax.min(mz + 1, last)))
    norm = jnp.zeros((8, LANES), jnp.float32)
    for o in range(2 * HALO + 1):
        shift = (HALO - o) % LANES
        near = pltpu.roll(places, shift, 1) if shift else places
        at = mz * block + lane + (o - HALO)
        keep = (at >= 0) & (at < total) & (abs(o - HALO) <= reach)
        c = jnp.where(keep, jnp.exp(-jnp.abs(near - places) / band_width), 0.0)
        band[o] = c
        norm = norm + c
    band[2 * HALO + 1] = jnp.where(lane < block, norm, 1.0)
    lamg[0] = lam_ref[...]

    def greet(mask):
        return pltpu.make_async_remote_copy(
            src_ref=lam_ref, dst_ref=lamg.at[mask], send_sem=es.at[0], recv_sem=er.at[0],
            device_id={"samp": flipped(mask)}, device_id_type=MESH)

    def chain(d, i):
        return pltpu.make_async_remote_copy(
            src_ref=sent.at[d, i], dst_ref=landed.at[d, i], send_sem=zs.at[d], recv_sem=zr.at[d, i],
            device_id={"cpg": lax.min(mz + 1, last) if d else lax.max(mz - 1, 0)}, device_id_type=MESH)

    def hand(d, j, c, cb):
        slot = mask_of(d, j) | cb
        return pltpu.make_async_remote_copy(
            src_ref=sent.at[d, j * chunks + c, pl.ds(cb * pair, pair)], dst_ref=full.at[slot, c],
            send_sem=hs.at[0], recv_sem=hr.at[slot],
            device_id={"samp": flipped(slot)}, device_id_type=MESH)

    def deliver(d, i, options):
        for j in options:
            @pl.when(lax.div(i, chunks) == j)
            def _():
                c = i - j * chunks
                if j == 0:
                    full[0, c] = sent[d, i, 0:pair, :]
                    hand(d, 0, c, 1).start()
                elif j == phases - 1:
                    for cb in range(2):
                        hand(d, j, c, cb).start()
                elif j == phases - 2:
                    for held in range(1, phases - 1):
                        for cb in range(2):
                            hand(d, held, c, cb).start()

    def advance(d, i, first, end, options):
        def own():
            return part[i, pl.ds(d * side, side), :]

        @pl.when(first)
        def _():
            sent[d, i] = own().astype(jnp.bfloat16)
            chain(d, i).start()

        @pl.when(jnp.logical_not(first))
        def _():
            chain(d, i).wait_recv()
            sent[d, i] = (own() + landed[d, i].astype(jnp.float32)).astype(jnp.bfloat16)

            @pl.when(jnp.logical_not(end))
            def _():
                chain(d, i).start()

            if options:
                @pl.when(end)
                def _():
                    deliver(d, i, options)

    lag = SKEW * last

    def forward(t, low, high):
        options = [j for j in range(phases) if low - lag < (j + 1) * chunks and high - lag > j * chunks]
        for d, behind in ((1, mz), (0, last - mz)):
            i = t - SKEW * behind
            with jax.named_scope("up" if d else "down"):
                if low >= lag and high <= units:
                    advance(d, i, behind == 0, behind == last, options)
                else:
                    @pl.when((i >= 0) & (i < units))
                    def _():
                        advance(d, i, behind == 0, behind == last, options)

    def phase(j):
        with jax.named_scope("sharewait"):
            for h in range(2):
                shared(h, j).wait_recv()
        if j == phases - 1:
            @pl.when(is_end)
            def _():
                for mask in range(1, n):
                    greet(mask).start()

        def step(c, carry):
            t = j * chunks + c
            if j == 0:
                load(c).wait()

                @pl.when(c + AHEAD < chunks)
                def _():
                    load(c + AHEAD).start()
            with jax.named_scope("mm"):
                part[t] = jnp.dot(g[j], v[c], preferred_element_type=jnp.float32)
            forward(t, j * chunks, (j + 1) * chunks)
            nxt = j + 1
            if nxt < phases:
                q = lax.div(c, 2)
                for h in range(2):
                    @pl.when(lax.rem(c, 2) == h)
                    def _():
                        top = top_of(nxt)
                        with jax.named_scope("shipwait"):
                            ship(h, nxt - (1 << top), nxt, q, orders[h][top]).wait_recv()
                        share(h, nxt, q).start()
                        after = nxt + 1
                        if after < phases:
                            upper = top_of(after)
                            turned = orders[1 - h][upper] == orders[h][top] and orders[h][upper] != orders[h][top]
                            k = 1 - h if turned else h
                            ship(k, after - (1 << upper), after, q, orders[k][upper]).start()
            return carry

        lax.fori_loop(0, chunks, step, 0)

    for j in range(phases):
        phase(j)

    def trail(t, carry):
        forward(t, units, units + lag)
        return carry

    lax.fori_loop(units, units + lag, trail, 0)

    row = lax.broadcasted_iota(jnp.int32, (half, LANES), 0)
    lane_of = lax.broadcasted_iota(jnp.int32, (half, LANES), 1)
    which = (mz == last).astype(jnp.int32)
    base = me * each + which * half
    home = lax.div(base, block)
    slot_mine = 2 * me + which
    per = block // half

    def post(step, i):
        return pltpu.make_async_remote_copy(
            src_ref=mail, dst_ref=got.at[slot_mine], send_sem=bs.at[step], recv_sem=br.at[2 - step],
            device_id={"samp": lax.rem(me + i, n), "cpg": lax.clamp(0, home + step - 1, last)}, device_id_type=MESH)

    def each_post(act):
        for step in range(3):
            plane = home + step - 1

            @pl.when((plane >= 0) & (plane <= last))
            def _():
                def body(i, carry):
                    @pl.when((i > 0) | (plane != mz))
                    def _():
                        act(post(step, i))
                    return carry

                lax.fori_loop(0, n, body, 0)

    def fold(x):
        return sum(x[:, k * LANES : (k + 1) * LANES] for k in range(CHUNK // LANES))

    def tall(x):
        return jnp.concatenate([x] * (half // 8), axis=0)

    def settle(acc):
        return [jnp.sum(x, axis=1, keepdims=True) for x in acc]

    def newton(log_scale, acc):
        crossed, energy, traced, fisher, s_r, s_p, s_q = settle(acc)
        effect = crossed / (energy + EPSILON)
        spread = s_r - 2.0 * effect * s_p + effect * effect * s_q
        gradient = 0.5 * (spread - traced)
        return log_scale + jnp.tanh(gradient / (jnp.exp(log_scale) * (0.5 * fisher)))

    @pl.when(is_end)
    def _():
        others = lamg.at[pl.ds(1, n - 1)]
        pltpu.make_async_remote_copy(
            src_ref=others, dst_ref=others, send_sem=es.at[0], recv_sem=er.at[0],
            device_id={"samp": flipped(1)}, device_id_type=MESH).wait_recv()
        acc = tuple(jnp.zeros((half if k < 5 else 8, LANES), jnp.float32) for k in range(7))
        for j in range(phases):
            for cb in range(2):
                here = j == 0 and cb == 0
                slot = jnp.where(mz == 0, mask_of(0, j) + cb, mask_of(1, j) + cb)

                if not here:
                    pltpu.make_async_remote_copy(
                        src_ref=full.at[slot], dst_ref=full.at[slot], send_sem=hs.at[0], recv_sem=hr.at[slot],
                        device_id={"samp": flipped(1)}, device_id_type=MESH).wait_recv()

                def absorb(c, acc):
                    at = slot * chunks + c
                    a = full[slot, c, 0:half, :].astype(jnp.float32)
                    b = full[slot, c, half:pair, :].astype(jnp.float32)
                    p, q, r = a * b, b * b, a * a
                    pp[at] = p
                    qq[at] = q
                    rr[at] = r
                    lam = lamg[slot, 0:1, pl.ds(pl.multiple_of(c * CHUNK, CHUNK), CHUNK)]
                    lam = jnp.broadcast_to(lam, (8, CHUNK))
                    lb[at] = lam
                    inv = 1.0 / (lam + 1.0)
                    lev = lam * inv
                    s = tall(lev * inv)
                    inv = tall(inv)
                    terms = (p * inv, q * inv, s * r, s * p, s * q, lev, lev * lev)
                    return tuple(x + fold(y) for x, y in zip(acc, terms))

                with jax.named_scope(f"absorb{2*j+cb}"):
                    acc = lax.fori_loop(0, chunks, absorb, acc)
        crossed, energy, s_r, s_p, s_q, traced, fisher = acc
        log_scale = newton(jnp.zeros((half, 1), jnp.float32),
                           (crossed, energy, tall(traced), tall(fisher), s_r, s_p, s_q))

        def sweep(log_scale, whole):
            scale = jnp.broadcast_to(jnp.exp(log_scale), (half, CHUNK))

            def terms_of(i):
                lam = tall(lb[i])
                inv = 1.0 / (scale * lam + 1.0)
                p = pp[i] * inv
                q = qq[i] * inv
                terms = [p, q]
                if whole:
                    lev = lam * inv
                    terms += [lev, lev * lev, rr[i] * (lev * inv), p * lev, q * lev]
                return [fold(y) for y in terms]

            def body(i, acc):
                for u in range(UNROLL):
                    acc = tuple(x + y for x, y in zip(acc, terms_of(i * UNROLL + u)))
                return acc

            start = tuple(jnp.zeros((half, LANES), jnp.float32) for _ in range(7 if whole else 2))
            return lax.fori_loop(0, n * chunks // UNROLL, body, start)

        for _ in range(ITERS - 1):
            with jax.named_scope("iter"):
                log_scale = newton(log_scale, sweep(log_scale, True))
        with jax.named_scope("lastsweep"):
            crossed, energy = settle(sweep(log_scale, False))
        zscore = crossed / jnp.sqrt(energy + EPSILON)
        hit = lane_of == row + lax.rem(base, block)
        mail[0:1, :] = jnp.sum(jnp.where(hit, jnp.broadcast_to(zscore, (half, LANES)), 0.0), axis=0, keepdims=True)
        mail[1:2, :] = jnp.sum(jnp.where(hit, jnp.broadcast_to(log_scale, (half, LANES)), 0.0), axis=0, keepdims=True)
        with jax.named_scope("post"):
            each_post(lambda copy: copy.start())

        @pl.when((home >= mz - 1) & (home <= mz + 1))
        def _():
            got[slot_mine] = mail[...]

    cur = jnp.zeros((2, LANES), jnp.float32)
    before = cur
    after = cur

    def letters(k, count):
        some = got.at[pl.ds(0, count)]
        return pltpu.make_async_remote_copy(
            src_ref=some, dst_ref=some, send_sem=bs.at[k], recv_sem=br.at[k],
            device_id={"samp": flipped(1)}, device_id_type=MESH)

    for k in range(3):
        near = (mz + k - 1 >= 0) & (mz + k - 1 <= last)
        inside = is_end & (home == mz + k - 1)
        with jax.named_scope("gotwait"):
            @pl.when(near & inside)
            def _():
                letters(k, per - 1).wait_recv()

            @pl.when(near & jnp.logical_not(inside))
            def _():
                letters(k, per).wait_recv()

    for h in range(2):
        for s in range(n):
            spot = (s * each + h * half) // block
            value = got[2 * s + h]
            cur = cur + jnp.where(mz == spot, value, 0.0)
            before = before + jnp.where(mz - 1 == spot, value, 0.0)
            after = after + jnp.where(mz + 1 == spot, value, 0.0)

    def tile(x, k):
        return jnp.broadcast_to(x[k : k + 1, :], (8, LANES))

    wide = spread_out(tile(cur, 0), tile(before, 0), tile(after, 0))
    acc = jnp.zeros((8, LANES), jnp.float32)
    for o in range(2 * HALO + 1):
        shift = (HALO - o) % LANES
        near = pltpu.roll(wide, shift, 1) if shift else wide
        acc = acc + band[o] * near
    top = lax.broadcasted_iota(jnp.int32, (8, LANES), 0)
    out_ref[...] = jnp.where(top == 0, acc / band[2 * HALO + 1], tile(cur, 1))

    for h in range(2):
        first = g.at[pl.ds(1, phases - 1), rows_of(h, 0)]
        pltpu.make_async_remote_copy(
            src_ref=first, dst_ref=first, send_sem=gs.at[h], recv_sem=gr.at[h, 0, 0],
            device_id={"samp": flipped(1)}, device_id_type=MESH).wait_send()
        every = g.at[:, rows_of(h, 0)]
        pltpu.make_async_remote_copy(
            src_ref=every, dst_ref=every, send_sem=ls.at[h], recv_sem=lr.at[h, 0],
            device_id={"samp": flipped(1)}, device_id_type=MESH).wait_send()

    def passed(d):
        return pltpu.make_async_remote_copy(
            src_ref=sent.at[d], dst_ref=landed.at[d], send_sem=zs.at[d], recv_sem=zr.at[d, 0],
            device_id={"samp": flipped(1)}, device_id_type=MESH)

    @pl.when(mz < last)
    def _():
        passed(1).wait_send()

    @pl.when(mz > 0)
    def _():
        passed(0).wait_send()

    @pl.when(is_end)
    def _():
        others = lamg.at[pl.ds(1, n - 1)]
        pltpu.make_async_remote_copy(
            src_ref=others, dst_ref=others, send_sem=es.at[0], recv_sem=er.at[0],
            device_id={"samp": flipped(1)}, device_id_type=MESH).wait_send()
        handed = full.at[pl.ds(1, n - 1)]
        pltpu.make_async_remote_copy(
            src_ref=handed, dst_ref=handed, send_sem=hs.at[0], recv_sem=hr.at[0],
            device_id={"samp": flipped(1)}, device_id_type=MESH).wait_send()
        for k in range(3):
            plane = home + k - 1

            @pl.when((plane >= 0) & (plane <= last) & (plane != mz))
            def _():
                letters(k, n).wait_send()

            @pl.when(plane == mz)
            def _():
                letters(k, n - 1).wait_send()


def scores(weights, responses, phenotype, eigvecs, eigvals, positions, reaches, n, cpgs):
    each, samples = weights.shape
    comps = eigvecs.shape[1]
    chunks = comps // CHUNK
    phases = n // 2
    units = phases * chunks
    half = each // 2
    pair = 2 * half
    side = 2 * pair
    total = each * n
    pieces = max(chunks // 2, 1)
    vmem = pl.BlockSpec(memory_space=pltpu.VMEM)
    hbm = pl.BlockSpec(memory_space=pl.ANY)
    dma = pltpu.SemaphoreType.DMA
    travel = pltpu.VMEM((2, units, side, CHUNK), jnp.bfloat16)
    big = pltpu.VMEM((n * chunks, half, CHUNK), jnp.float32)
    return pl.pallas_call(
        functools.partial(score_kernel, n, cpgs),
        out_shape=jax.ShapeDtypeStruct((8, LANES), jnp.float32),
        in_specs=[hbm, hbm, vmem, hbm, vmem, vmem, vmem],
        out_specs=vmem,
        scratch_shapes=[
            pltpu.VMEM((each, samples), jnp.bfloat16),
            pltpu.VMEM((each, samples), jnp.bfloat16),
            pltpu.VMEM((phases, 2 * side, samples), jnp.bfloat16),
            pltpu.VMEM((chunks, samples, CHUNK), jnp.bfloat16),
            pltpu.VMEM((units, 2 * side, CHUNK), jnp.float32),
            travel, travel,
            pltpu.VMEM((n, chunks, pair, CHUNK), jnp.bfloat16),
            big, big, big,
            pltpu.VMEM((n * chunks, 8, CHUNK), jnp.float32),
            pltpu.VMEM((n, 1, comps), jnp.float32),
            pltpu.VMEM((2, LANES), jnp.float32),
            pltpu.VMEM((2 * n, 2, LANES), jnp.float32),
            pltpu.VMEM((8, LANES), jnp.int32),
            pltpu.VMEM((2 * HALO + 2, 8, LANES), jnp.float32),
            dma((2,)), dma((chunks,)),
            dma((2,)), dma((2, phases, pieces)),
            dma((2,)), dma((2, phases)),
            dma((2,)), dma((2, units)),
            dma((1,)), dma((n,)),
            dma((1,)), dma((1,)),
            dma((3,)), dma((3,)),
        ],
        compiler_params=pltpu.CompilerParams(collective_id=1, has_side_effects=True, vmem_limit_bytes=60 * 1024 * 1024),
        cost_estimate=pl.CostEstimate(flops=4 * total * samples * comps, bytes_accessed=2 * samples * comps, transcendentals=0),
        name="scores",
    )(weights, responses, phenotype[None, :], eigvecs, eigvals[None, :], positions[None, :], reaches[None, :])


def shards(responses, weights, phenotype, eigvecs, eigvals, positions, reaches):
    n, cpgs = lax.axis_size("samp"), lax.axis_size("cpg")
    out = scores(weights, responses, phenotype, eigvecs, eigvals, positions, reaches, n, cpgs)
    block = reaches.shape[0]
    return (out[0, :block], out[1, :block])


def solution(mesh):
    in_specs = (P("samp", "cpg"), P("samp", "cpg"), P("cpg"), P("cpg", "samp"), P("samp"), P(), P("cpg"))
    out_specs = (P("cpg"), P("cpg"))
    return jax.shard_map(shards, mesh=mesh, in_specs=in_specs, out_specs=out_specs, check_vma=False)
```

```python
import functools

import jax
import jax.numpy as jnp
from jax import lax
from jax.experimental import pallas as pl
from jax.experimental.pallas import tpu as pltpu
from jax.sharding import PartitionSpec as P

ITERS = 4
HALO = 8
EPSILON = 1e-06
band_width = 1000.0
MESH = pl.DeviceIdType.MESH
LANES = 128
CHUNK = 256
SKEW = 5
STRIP = 512
AHEAD = 3
UNROLL = 4


def score_kernel(n, cpgs, w_hbm, r_hbm, ph_hbm, v_hbm, lam_hbm, pos_hbm, reach_hbm, out_ref,
                 wbuf, rbuf, g, v, part, sent, landed, full, pp, qq, rr, lb, lamg, mail, got, pad, band, ph_ref, lam_ref, pos_ref, reach_ref,
                 wsem, vsem, gs, gr, ls, lr, zs, zr, hs, hr, es, er, bs, br):
    me = lax.axis_index("samp")
    mz = lax.axis_index("cpg")
    last = cpgs - 1
    each, samples = wbuf.shape
    half = each // 2
    pair = 2 * half
    side = 2 * pair
    phases = g.shape[0]
    chunks = v.shape[0]
    units = phases * chunks
    total = each * n
    block = total // cpgs
    bits = [1 << i for i in range(1, n.bit_length() - 1)]
    orders = (bits, bits[::-1])
    pieces = gr.shape[2]
    cols = samples // pieces
    is_end = (mz == 0) | (mz == last)

    def mask_of(h, j):
        return sum(bit for i, bit in enumerate(orders[h]) if (j >> i) & 1)

    def flipped(mask):
        out = me
        bit = 1
        while bit <= mask:
            if mask & bit:
                out = out + bit - 2 * bit * lax.rem(lax.div(me, bit), 2)
            bit *= 2
        return out

    moves = ((w_hbm, wbuf), (r_hbm, rbuf), (ph_hbm, ph_ref), (pos_hbm, pos_ref), (reach_hbm, reach_ref), (lam_hbm, lam_ref))
    loads = [pltpu.make_async_copy(src, dst, wsem.at[k]) for k, (src, dst) in enumerate(moves)]
    for c in loads:
        c.start()

    def load(c):
        return pltpu.make_async_copy(v_hbm.at[:, pl.ds(pl.multiple_of(c * CHUNK, CHUNK), CHUNK)], v.at[c], vsem.at[lax.rem(c, AHEAD)])

    got[...] = jnp.zeros_like(got)
    barrier = pltpu.get_barrier_semaphore()
    for j in range(1, n):
        pl.semaphore_signal(barrier, inc=1, device_id={"samp": flipped(j)}, device_id_type=MESH)

    @pl.when(mz > 0)
    def _():
        pl.semaphore_signal(barrier, inc=1, device_id={"cpg": lax.max(mz - 1, 0)}, device_id_type=MESH)

    @pl.when(mz < last)
    def _():
        pl.semaphore_signal(barrier, inc=1, device_id={"cpg": lax.min(mz + 1, last)}, device_id_type=MESH)

    with jax.named_scope("loadwait"):
        for c in loads[:3]:
            c.wait()
    for c in range(min(AHEAD, chunks)):
        load(c).start()

    def rows_of(h, cb):
        return pl.ds(h * side + cb * pair, pair)

    def prepare(i, carry):
        at = pl.ds(pl.multiple_of(i * STRIP, STRIP), STRIP)
        root = jnp.sqrt(wbuf[:, at].astype(jnp.float32))
        weighted = (root * rbuf[:, at].astype(jnp.float32)).astype(jnp.bfloat16)
        design = (root * ph_ref[:, at]).astype(jnp.bfloat16)
        for h in range(2):
            g[0, pl.ds(h * side, half), at] = weighted[h * half : (h + 1) * half]
            g[0, pl.ds(h * side + half, half), at] = design[h * half : (h + 1) * half]
        return carry

    with jax.named_scope("prep"):
        lax.fori_loop(0, samples // STRIP, prepare, 0)

    def piece(q):
        return pl.ds(pl.multiple_of(q * cols, cols), cols)

    def ship(h, src, dst, q, bit):
        return pltpu.make_async_remote_copy(
            src_ref=g.at[src, rows_of(h, 0), piece(q)], dst_ref=g.at[dst, rows_of(h, 0), piece(q)],
            send_sem=gs.at[0], recv_sem=gr.at[h, dst - 1, q],
            device_id={"samp": flipped(bit)}, device_id_type=MESH)

    def share(h, j, q):
        return pltpu.make_async_remote_copy(
            src_ref=g.at[j, rows_of(h, 0), piece(q)], dst_ref=g.at[j, rows_of(h, 1), piece(q)],
            send_sem=ls.at[0], recv_sem=lr.at[j],
            device_id={"samp": flipped(1)}, device_id_type=MESH)

    pl.semaphore_wait(barrier, n - 1 + (mz > 0).astype(jnp.int32) + (mz < last).astype(jnp.int32))

    for q in range(pieces):
        for h in range(2):
            ship(h, 0, 1, q, orders[h][0]).start()
    for q in range(pieces):
        for h in range(2):
            share(h, 0, q).start()

    def shared(j):
        both = g.at[j, pl.ds(0, side)]
        return pltpu.make_async_remote_copy(
            src_ref=both, dst_ref=both, send_sem=ls.at[0], recv_sem=lr.at[j],
            device_id={"samp": flipped(1)}, device_id_type=MESH)

    def top_of(j):
        return j.bit_length() - 1

    for c in loads[3:]:
        c.wait()
    lane = lax.broadcasted_iota(jnp.int32, (8, LANES), 1)

    def spread_out(cur, before, after):
        right = pltpu.roll(after, block, 1)
        left = pltpu.roll(before, LANES - block, 1)
        return jnp.where(lane < block, cur, jnp.where(lane < block + HALO, right, left))

    def spots(b):
        at = b * block
        row = pos_ref[0:1, pl.ds(pl.multiple_of(lax.div(at, LANES) * LANES, LANES), LANES)].astype(jnp.float32)
        return pltpu.roll(jnp.broadcast_to(row, (8, LANES)), lax.rem(LANES - lax.rem(at, LANES), LANES), 1)

    pad[...] = jnp.zeros_like(pad)
    pad[0:1, 0:block] = reach_ref[...]
    reach = jnp.broadcast_to(pad[0:1, :], (8, LANES))
    places = spread_out(spots(mz), spots(lax.max(mz - 1, 0)), spots(lax.min(mz + 1, last)))
    norm = jnp.zeros((8, LANES), jnp.float32)
    for o in range(2 * HALO + 1):
        shift = (HALO - o) % LANES
        near = pltpu.roll(places, shift, 1) if shift else places
        at = mz * block + lane + (o - HALO)
        keep = (at >= 0) & (at < total) & (abs(o - HALO) <= reach)
        c = jnp.where(keep, jnp.exp(-jnp.abs(near - places) / band_width), 0.0)
        band[o] = c
        norm = norm + c
    band[2 * HALO + 1] = jnp.where(lane < block, norm, 1.0)
    lamg[0] = lam_ref[...]

    def greet(mask):
        return pltpu.make_async_remote_copy(
            src_ref=lam_ref, dst_ref=lamg.at[mask], send_sem=es.at[0], recv_sem=er.at[0],
            device_id={"samp": flipped(mask)}, device_id_type=MESH)

    def chain(d, i):
        return pltpu.make_async_remote_copy(
            src_ref=sent.at[d, i], dst_ref=landed.at[d, i], send_sem=zs.at[d], recv_sem=zr.at[d, i],
            device_id={"cpg": lax.min(mz + 1, last) if d else lax.max(mz - 1, 0)}, device_id_type=MESH)

    def hand(d, j, c, cb):
        slot = mask_of(d, phases - 1 - j) | cb
        return pltpu.make_async_remote_copy(
            src_ref=sent.at[d, j * chunks + c, pl.ds(cb * pair, pair)], dst_ref=full.at[slot, c],
            send_sem=hs.at[0], recv_sem=hr.at[slot],
            device_id={"samp": flipped(slot)}, device_id_type=MESH)

    def deliver(d, i, options):
        for j in options:
            @pl.when(lax.div(i, chunks) == j)
            def _():
                c = i - j * chunks
                if j == phases - 1:
                    full[0, c] = sent[d, i, 0:pair, :]
                    hand(d, j, c, 1).start()
                elif j:
                    for held in ((0, 1) if j == 1 else (j,)):
                        for cb in range(2):
                            hand(d, held, c, cb).start()

    def advance(d, i, first, end, options):
        def own():
            return part[i, pl.ds(d * side, side), :]

        @pl.when(first)
        def _():
            sent[d, i] = own().astype(jnp.bfloat16)
            chain(d, i).start()

        @pl.when(jnp.logical_not(first))
        def _():
            chain(d, i).wait_recv()
            sent[d, i] = (own() + landed[d, i].astype(jnp.float32)).astype(jnp.bfloat16)

            @pl.when(jnp.logical_not(end))
            def _():
                chain(d, i).start()

            if options:
                @pl.when(end)
                def _():
                    deliver(d, i, options)

    lag = SKEW * last

    def forward(t, low, high):
        options = [j for j in range(phases) if low - lag < (j + 1) * chunks and high - lag > j * chunks]
        for d, behind in ((1, mz), (0, last - mz)):
            i = t - SKEW * behind
            with jax.named_scope("up" if d else "down"):
                if low >= lag and high <= units:
                    advance(d, i, behind == 0, behind == last, options)
                else:
                    @pl.when((i >= 0) & (i < units))
                    def _():
                        advance(d, i, behind == 0, behind == last, options)

    def phase(j):
        with jax.named_scope("sharewait"):
            shared(j).wait_recv()
        if j == phases - 1:
            @pl.when(is_end)
            def _():
                for mask in range(1, n):
                    greet(mask).start()

        def step(c, carry):
            t = j * chunks + c
            if j == 0:
                load(c).wait()

                @pl.when(c + AHEAD < chunks)
                def _():
                    load(c + AHEAD).start()
            with jax.named_scope("mm"):
                part[t] = jnp.dot(g[j], v[c], preferred_element_type=jnp.float32)
            forward(t, j * chunks, (j + 1) * chunks)
            nxt = j + 1
            if nxt < phases:
                q = lax.div(c, 2)
                for h in range(2):
                    @pl.when(lax.rem(c, 2) == h)
                    def _():
                        top = top_of(nxt)
                        with jax.named_scope("shipwait"):
                            ship(h, nxt - (1 << top), nxt, q, orders[h][top]).wait_recv()
                        share(h, nxt, q).start()
                        after = nxt + 1
                        if after < phases:
                            upper = top_of(after)
                            turned = orders[1 - h][upper] == orders[h][top] and orders[h][upper] != orders[h][top]
                            k = 1 - h if turned else h
                            ship(k, after - (1 << upper), after, q, orders[k][upper]).start()
            return carry

        lax.fori_loop(0, chunks, step, 0)

    for j in range(phases):
        phase(j)

    def trail(t, carry):
        forward(t, units, units + lag)
        return carry

    lax.fori_loop(units, units + lag, trail, 0)

    row = lax.broadcasted_iota(jnp.int32, (half, LANES), 0)
    lane_of = lax.broadcasted_iota(jnp.int32, (half, LANES), 1)
    which = (mz == last).astype(jnp.int32)
    source = flipped(sum(bits))
    base = source * each + which * half
    home = lax.div(base, block)
    slot_mine = 2 * source + which
    per = block // half

    def post(step, i):
        return pltpu.make_async_remote_copy(
            src_ref=mail, dst_ref=got.at[slot_mine], send_sem=bs.at[step], recv_sem=br.at[2 - step],
            device_id={"samp": lax.rem(me + i, n), "cpg": lax.clamp(0, home + step - 1, last)}, device_id_type=MESH)

    def each_post(act):
        for step in range(3):
            plane = home + step - 1

            @pl.when((plane >= 0) & (plane <= last))
            def _():
                def body(i, carry):
                    @pl.when((i > 0) | (plane != mz))
                    def _():
                        act(post(step, i))
                    return carry

                lax.fori_loop(0, n, body, 0)

    def fold(x):
        return sum(x[:, k * LANES : (k + 1) * LANES] for k in range(CHUNK // LANES))

    def tall(x):
        return jnp.concatenate([x] * (half // 8), axis=0)

    def settle(acc):
        return [jnp.sum(x, axis=1, keepdims=True) for x in acc]

    def newton(log_scale, acc):
        crossed, energy, traced, fisher, s_r, s_p, s_q = settle(acc)
        effect = crossed / (energy + EPSILON)
        spread = s_r - 2.0 * effect * s_p + effect * effect * s_q
        gradient = 0.5 * (spread - traced)
        return log_scale + jnp.tanh(gradient / (jnp.exp(log_scale) * (0.5 * fisher)))

    @pl.when(is_end)
    def _():
        others = lamg.at[pl.ds(1, n - 1)]
        pltpu.make_async_remote_copy(
            src_ref=others, dst_ref=others, send_sem=es.at[0], recv_sem=er.at[0],
            device_id={"samp": flipped(1)}, device_id_type=MESH).wait_recv()
        acc = tuple(jnp.zeros((half if k < 5 else 8, LANES), jnp.float32) for k in range(7))
        for j in range(phases):
            for cb in range(2):
                here = j == phases - 1 and cb == 0
                slot = jnp.where(mz == 0, mask_of(0, phases - 1 - j) + cb, mask_of(1, phases - 1 - j) + cb)

                if not here:
                    pltpu.make_async_remote_copy(
                        src_ref=full.at[slot], dst_ref=full.at[slot], send_sem=hs.at[0], recv_sem=hr.at[slot],
                        device_id={"samp": flipped(1)}, device_id_type=MESH).wait_recv()

                def absorb(c, acc):
                    at = slot * chunks + c
                    a = full[slot, c, 0:half, :].astype(jnp.float32)
                    b = full[slot, c, half:pair, :].astype(jnp.float32)
                    p, q, r = a * b, b * b, a * a
                    pp[at] = p
                    qq[at] = q
                    rr[at] = r
                    lam = lamg[slot, 0:1, pl.ds(pl.multiple_of(c * CHUNK, CHUNK), CHUNK)]
                    lam = jnp.broadcast_to(lam, (8, CHUNK))
                    lb[at] = lam
                    inv = 1.0 / (lam + 1.0)
                    lev = lam * inv
                    s = tall(lev * inv)
                    inv = tall(inv)
                    terms = (p * inv, q * inv, s * r, s * p, s * q, lev, lev * lev)
                    return tuple(x + fold(y) for x, y in zip(acc, terms))

                with jax.named_scope(f"absorb{2*j+cb}"):
                    acc = lax.fori_loop(0, chunks, absorb, acc)
        crossed, energy, s_r, s_p, s_q, traced, fisher = acc
        log_scale = newton(jnp.zeros((half, 1), jnp.float32),
                           (crossed, energy, tall(traced), tall(fisher), s_r, s_p, s_q))

        def sweep(log_scale, whole):
            scale = jnp.broadcast_to(jnp.exp(log_scale), (half, CHUNK))

            def terms_of(i):
                lam = tall(lb[i])
                inv = 1.0 / (scale * lam + 1.0)
                p = pp[i] * inv
                q = qq[i] * inv
                terms = [p, q]
                if whole:
                    lev = lam * inv
                    terms += [lev, lev * lev, rr[i] * (lev * inv), p * lev, q * lev]
                return [fold(y) for y in terms]

            def body(i, acc):
                for u in range(UNROLL):
                    acc = tuple(x + y for x, y in zip(acc, terms_of(i * UNROLL + u)))
                return acc

            start = tuple(jnp.zeros((half, LANES), jnp.float32) for _ in range(7 if whole else 2))
            return lax.fori_loop(0, n * chunks // UNROLL, body, start)

        for _ in range(ITERS - 1):
            with jax.named_scope("iter"):
                log_scale = newton(log_scale, sweep(log_scale, True))
        with jax.named_scope("lastsweep"):
            crossed, energy = settle(sweep(log_scale, False))
        zscore = crossed / jnp.sqrt(energy + EPSILON)
        hit = lane_of == row + lax.rem(base, block)
        mail[0:1, :] = jnp.sum(jnp.where(hit, jnp.broadcast_to(zscore, (half, LANES)), 0.0), axis=0, keepdims=True)
        mail[1:2, :] = jnp.sum(jnp.where(hit, jnp.broadcast_to(log_scale, (half, LANES)), 0.0), axis=0, keepdims=True)
        with jax.named_scope("post"):
            each_post(lambda copy: copy.start())

        @pl.when((home >= mz - 1) & (home <= mz + 1))
        def _():
            got[slot_mine] = mail[...]

    cur = jnp.zeros((2, LANES), jnp.float32)
    before = cur
    after = cur

    def letters(k, count):
        some = got.at[pl.ds(0, count)]
        return pltpu.make_async_remote_copy(
            src_ref=some, dst_ref=some, send_sem=bs.at[k], recv_sem=br.at[k],
            device_id={"samp": flipped(1)}, device_id_type=MESH)

    for k in range(3):
        near = (mz + k - 1 >= 0) & (mz + k - 1 <= last)
        inside = is_end & (home == mz + k - 1)
        with jax.named_scope("gotwait"):
            @pl.when(near & inside)
            def _():
                letters(k, per - 1).wait_recv()

            @pl.when(near & jnp.logical_not(inside))
            def _():
                letters(k, per).wait_recv()

    for h in range(2):
        for s in range(n):
            spot = (s * each + h * half) // block
            value = got[2 * s + h]
            cur = cur + jnp.where(mz == spot, value, 0.0)
            before = before + jnp.where(mz - 1 == spot, value, 0.0)
            after = after + jnp.where(mz + 1 == spot, value, 0.0)

    def tile(x, k):
        return jnp.broadcast_to(x[k : k + 1, :], (8, LANES))

    wide = spread_out(tile(cur, 0), tile(before, 0), tile(after, 0))
    acc = jnp.zeros((8, LANES), jnp.float32)
    for o in range(2 * HALO + 1):
        shift = (HALO - o) % LANES
        near = pltpu.roll(wide, shift, 1) if shift else wide
        acc = acc + band[o] * near
    top = lax.broadcasted_iota(jnp.int32, (8, LANES), 0)
    out_ref[...] = jnp.where(top == 0, acc / band[2 * HALO + 1], tile(cur, 1))

    first = g.at[pl.ds(1, phases - 1), pl.ds(0, side)]
    pltpu.make_async_remote_copy(
        src_ref=first, dst_ref=first, send_sem=gs.at[0], recv_sem=gr.at[0, 0, 0],
        device_id={"samp": flipped(1)}, device_id_type=MESH).wait_send()
    every = g.at[:, pl.ds(0, side)]
    pltpu.make_async_remote_copy(
        src_ref=every, dst_ref=every, send_sem=ls.at[0], recv_sem=lr.at[0],
        device_id={"samp": flipped(1)}, device_id_type=MESH).wait_send()

    def passed(d):
        return pltpu.make_async_remote_copy(
            src_ref=sent.at[d], dst_ref=landed.at[d], send_sem=zs.at[d], recv_sem=zr.at[d, 0],
            device_id={"samp": flipped(1)}, device_id_type=MESH)

    @pl.when(mz < last)
    def _():
        passed(1).wait_send()

    @pl.when(mz > 0)
    def _():
        passed(0).wait_send()

    @pl.when(is_end)
    def _():
        others = lamg.at[pl.ds(1, n - 1)]
        pltpu.make_async_remote_copy(
            src_ref=others, dst_ref=others, send_sem=es.at[0], recv_sem=er.at[0],
            device_id={"samp": flipped(1)}, device_id_type=MESH).wait_send()
        handed = full.at[pl.ds(1, n - 1)]
        pltpu.make_async_remote_copy(
            src_ref=handed, dst_ref=handed, send_sem=hs.at[0], recv_sem=hr.at[0],
            device_id={"samp": flipped(1)}, device_id_type=MESH).wait_send()
        for k in range(3):
            plane = home + k - 1

            @pl.when((plane >= 0) & (plane <= last) & (plane != mz))
            def _():
                letters(k, n).wait_send()

            @pl.when(plane == mz)
            def _():
                letters(k, n - 1).wait_send()


def scores(weights, responses, phenotype, eigvecs, eigvals, positions, reaches, n, cpgs):
    each, samples = weights.shape
    comps = eigvecs.shape[1]
    chunks = comps // CHUNK
    phases = n // 2
    units = phases * chunks
    half = each // 2
    pair = 2 * half
    side = 2 * pair
    total = each * n
    pieces = max(chunks // 2, 1)
    vmem = pl.BlockSpec(memory_space=pltpu.VMEM)
    hbm = pl.BlockSpec(memory_space=pl.ANY)
    dma = pltpu.SemaphoreType.DMA
    travel = pltpu.VMEM((2, units, side, CHUNK), jnp.bfloat16)
    big = pltpu.VMEM((n * chunks, half, CHUNK), jnp.float32)
    return pl.pallas_call(
        functools.partial(score_kernel, n, cpgs),
        out_shape=jax.ShapeDtypeStruct((8, LANES), jnp.float32),
        in_specs=[hbm] * 7,
        out_specs=vmem,
        scratch_shapes=[
            pltpu.VMEM((each, samples), jnp.bfloat16),
            pltpu.VMEM((each, samples), jnp.bfloat16),
            pltpu.VMEM((phases, 2 * side, samples), jnp.bfloat16),
            pltpu.VMEM((chunks, samples, CHUNK), jnp.bfloat16),
            pltpu.VMEM((units, 2 * side, CHUNK), jnp.float32),
            travel, travel,
            pltpu.VMEM((n, chunks, pair, CHUNK), jnp.bfloat16),
            big, big, big,
            pltpu.VMEM((n * chunks, 8, CHUNK), jnp.float32),
            pltpu.VMEM((n, 1, comps), jnp.float32),
            pltpu.VMEM((2, LANES), jnp.float32),
            pltpu.VMEM((2 * n, 2, LANES), jnp.float32),
            pltpu.VMEM((8, LANES), jnp.int32),
            pltpu.VMEM((2 * HALO + 2, 8, LANES), jnp.float32),
            pltpu.VMEM((1, samples), jnp.float32),
            pltpu.VMEM((1, comps), jnp.float32),
            pltpu.VMEM((1, total), jnp.int32),
            pltpu.VMEM((1, total // cpgs), jnp.int32),
            dma((6,)), dma((AHEAD,)),
            dma((1,)), dma((2, phases - 1, pieces)),
            dma((1,)), dma((phases,)),
            dma((2,)), dma((2, units)),
            dma((1,)), dma((n,)),
            dma((1,)), dma((1,)),
            dma((3,)), dma((3,)),
        ],
        compiler_params=pltpu.CompilerParams(collective_id=1, has_side_effects=True, vmem_limit_bytes=60 * 1024 * 1024),
        cost_estimate=pl.CostEstimate(flops=4 * total * samples * comps, bytes_accessed=2 * samples * comps, transcendentals=0),
        name="scores",
    )(weights, responses, phenotype[None, :], eigvecs, eigvals[None, :], positions[None, :], reaches[None, :])


def shards(responses, weights, phenotype, eigvecs, eigvals, positions, reaches):
    n, cpgs = lax.axis_size("samp"), lax.axis_size("cpg")
    out = scores(weights, responses, phenotype, eigvecs, eigvals, positions, reaches, n, cpgs)
    block = reaches.shape[0]
    return (out[0, :block], out[1, :block])


def solution(mesh):
    in_specs = (P("samp", "cpg"), P("samp", "cpg"), P("cpg"), P("cpg", "samp"), P("samp"), P(), P("cpg"))
    out_specs = (P("cpg"), P("cpg"))
    return jax.shard_map(shards, mesh=mesh, in_specs=in_specs, out_specs=out_specs, check_vma=False)
```

```python
import functools

import jax
import jax.numpy as jnp
from jax import lax
from jax.experimental import pallas as pl
from jax.experimental.pallas import tpu as pltpu
from jax.sharding import PartitionSpec as P

ITERS = 4
HALO = 8
EPSILON = 1e-06
band_width = 1000.0
MESH = pl.DeviceIdType.MESH
LANES = 128
CHUNK = 256
SKEW = 9
STRIP = 512
AHEAD = 3
UNROLL = 4


def score_kernel(n, cpgs, w_hbm, r_hbm, ph_hbm, v_hbm, lam_hbm, pos_hbm, reach_hbm, out_ref,
                 wbuf, rbuf, g, v, part, sent, landed, full, pp, qq, rr, lb, lamg, mail, got, pad, band, ph_ref, lam_ref, pos_ref, reach_ref,
                 wsem, vsem, gs, gr, ls, lr, zs, zr, hs, hr, es, er, bs, br):
    me = lax.axis_index("samp")
    mz = lax.axis_index("cpg")
    last = cpgs - 1
    each, samples = wbuf.shape
    half = each // 2
    pair = 2 * half
    side = 2 * pair
    phases = g.shape[0]
    chunks = v.shape[0]
    units = phases * chunks
    total = each * n
    block = total // cpgs
    bits = [1 << i for i in range(1, n.bit_length() - 1)]
    orders = (bits, bits[::-1])
    pieces = gr.shape[2]
    cols = samples // pieces
    is_end = (mz == 0) | (mz == last)

    def lag_of(d, k):
        turned = SKEW * k + (1 - d)
        return turned // 2 if isinstance(k, int) else lax.div(turned, 2)


    def mask_of(h, j):
        return sum(bit for i, bit in enumerate(orders[h]) if (j >> i) & 1)

    def flipped(mask):
        out = me
        bit = 1
        while bit <= mask:
            if mask & bit:
                out = out + bit - 2 * bit * lax.rem(lax.div(me, bit), 2)
            bit *= 2
        return out

    moves = ((w_hbm, wbuf), (r_hbm, rbuf), (ph_hbm, ph_ref), (pos_hbm, pos_ref), (reach_hbm, reach_ref), (lam_hbm, lam_ref))
    loads = [pltpu.make_async_copy(src, dst, wsem.at[k]) for k, (src, dst) in enumerate(moves)]
    for c in loads:
        c.start()

    def load(c):
        return pltpu.make_async_copy(v_hbm.at[:, pl.ds(pl.multiple_of(c * CHUNK, CHUNK), CHUNK)], v.at[c], vsem.at[lax.rem(c, AHEAD)])

    got[...] = jnp.zeros_like(got)
    barrier = pltpu.get_barrier_semaphore()
    for j in range(1, n):
        pl.semaphore_signal(barrier, inc=1, device_id={"samp": flipped(j)}, device_id_type=MESH)

    @pl.when(mz > 0)
    def _():
        pl.semaphore_signal(barrier, inc=1, device_id={"cpg": lax.max(mz - 1, 0)}, device_id_type=MESH)

    @pl.when(mz < last)
    def _():
        pl.semaphore_signal(barrier, inc=1, device_id={"cpg": lax.min(mz + 1, last)}, device_id_type=MESH)

    with jax.named_scope("loadwait"):
        for c in loads[:3]:
            c.wait()
    for c in range(min(AHEAD, chunks)):
        load(c).start()

    def rows_of(h, cb):
        return pl.ds(h * side + cb * pair, pair)

    def prepare(i, carry):
        at = pl.ds(pl.multiple_of(i * STRIP, STRIP), STRIP)
        root = jnp.sqrt(wbuf[:, at].astype(jnp.float32))
        weighted = (root * rbuf[:, at].astype(jnp.float32)).astype(jnp.bfloat16)
        design = (root * ph_ref[:, at]).astype(jnp.bfloat16)
        for h in range(2):
            g[0, pl.ds(h * side, half), at] = weighted[h * half : (h + 1) * half]
            g[0, pl.ds(h * side + half, half), at] = design[h * half : (h + 1) * half]
        return carry


    def piece(q):
        return pl.ds(pl.multiple_of(q * cols, cols), cols)

    def ship(h, src, dst, q, bit):
        return pltpu.make_async_remote_copy(
            src_ref=g.at[src, rows_of(h, 0), piece(q)], dst_ref=g.at[dst, rows_of(h, 0), piece(q)],
            send_sem=gs.at[0], recv_sem=gr.at[h, dst - 1, q],
            device_id={"samp": flipped(bit)}, device_id_type=MESH)

    def share(h, j, q):
        return pltpu.make_async_remote_copy(
            src_ref=g.at[j, rows_of(h, 0), piece(q)], dst_ref=g.at[j, rows_of(h, 1), piece(q)],
            send_sem=ls.at[0], recv_sem=lr.at[j],
            device_id={"samp": flipped(1)}, device_id_type=MESH)

    strips = cols // STRIP
    for q in range(pieces):
        lax.fori_loop(q * strips, (q + 1) * strips, prepare, 0)
        if q == 0:
            pl.semaphore_wait(barrier, n - 1 + (mz > 0).astype(jnp.int32) + (mz < last).astype(jnp.int32))
        for h in range(2):
            ship(h, 0, 1, q, orders[h][0]).start()
    for q in range(pieces):
        for h in range(2):
            share(h, 0, q).start()

    def shared(j):
        both = g.at[j, pl.ds(0, side)]
        return pltpu.make_async_remote_copy(
            src_ref=both, dst_ref=both, send_sem=ls.at[0], recv_sem=lr.at[j],
            device_id={"samp": flipped(1)}, device_id_type=MESH)

    def top_of(j):
        return j.bit_length() - 1

    for c in loads[3:]:
        c.wait()
    lane = lax.broadcasted_iota(jnp.int32, (8, LANES), 1)

    def spread_out(cur, before, after):
        right = pltpu.roll(after, block, 1)
        left = pltpu.roll(before, LANES - block, 1)
        return jnp.where(lane < block, cur, jnp.where(lane < block + HALO, right, left))

    def spots(b):
        at = b * block
        row = pos_ref[0:1, pl.ds(pl.multiple_of(lax.div(at, LANES) * LANES, LANES), LANES)].astype(jnp.float32)
        return pltpu.roll(jnp.broadcast_to(row, (8, LANES)), lax.rem(LANES - lax.rem(at, LANES), LANES), 1)

    pad[...] = jnp.zeros_like(pad)
    pad[0:1, 0:block] = reach_ref[...]
    reach = jnp.broadcast_to(pad[0:1, :], (8, LANES))
    places = spread_out(spots(mz), spots(lax.max(mz - 1, 0)), spots(lax.min(mz + 1, last)))
    norm = jnp.zeros((8, LANES), jnp.float32)
    for o in range(2 * HALO + 1):
        shift = (HALO - o) % LANES
        near = pltpu.roll(places, shift, 1) if shift else places
        at = mz * block + lane + (o - HALO)
        keep = (at >= 0) & (at < total) & (abs(o - HALO) <= reach)
        c = jnp.where(keep, jnp.exp(-jnp.abs(near - places) / band_width), 0.0)
        band[o] = c
        norm = norm + c
    band[2 * HALO + 1] = jnp.where(lane < block, norm, 1.0)
    lamg[0] = lam_ref[...]

    def greet(mask):
        return pltpu.make_async_remote_copy(
            src_ref=lam_ref, dst_ref=lamg.at[mask], send_sem=es.at[0], recv_sem=er.at[0],
            device_id={"samp": flipped(mask)}, device_id_type=MESH)

    def chain(d, i):
        return pltpu.make_async_remote_copy(
            src_ref=sent.at[d, i], dst_ref=landed.at[d, i], send_sem=zs.at[d], recv_sem=zr.at[d, lax.rem(i, zr.shape[1])],
            device_id={"cpg": lax.min(mz + 1, last) if d else lax.max(mz - 1, 0)}, device_id_type=MESH)

    def hand(d, j, c, cb):
        slot = mask_of(d, phases - 1 - j) | cb
        return pltpu.make_async_remote_copy(
            src_ref=sent.at[d, j * chunks + c, pl.ds(cb * pair, pair)], dst_ref=full.at[slot, c],
            send_sem=hs.at[0], recv_sem=hr.at[slot],
            device_id={"samp": flipped(slot)}, device_id_type=MESH)

    def deliver(d, i, options):
        for j in options:
            @pl.when(lax.div(i, chunks) == j)
            def _():
                c = i - j * chunks
                if j == phases - 1:
                    full[0, c] = sent[d, i, 0:pair, :]
                    hand(d, j, c, 1).start()
                elif j:
                    for held in ((0, 1) if j == 1 else (j,)):
                        for cb in range(2):
                            hand(d, held, c, cb).start()

    def advance(d, i, first, end, options):
        def own():
            return part[i, pl.ds(d * side, side), :]

        @pl.when(first)
        def _():
            sent[d, i] = own().astype(jnp.bfloat16)
            chain(d, i).start()

        @pl.when(jnp.logical_not(first))
        def _():
            chain(d, i).wait_recv()
            sent[d, i] = (own() + landed[d, i].astype(jnp.float32)).astype(jnp.bfloat16)

            @pl.when(jnp.logical_not(end))
            def _():
                chain(d, i).start()

            if options:
                @pl.when(end)
                def _():
                    deliver(d, i, options)

    lag = max(lag_of(0, last), lag_of(1, last))

    def forward(t, low, high):
        for d, behind in ((1, mz), (0, last - mz)):
            whole = lag_of(d, last)
            options = [j for j in range(phases) if low - whole < (j + 1) * chunks and high - whole > j * chunks]
            i = t - lag_of(d, behind)
            with jax.named_scope("up" if d else "down"):
                if low >= lag and high <= units:
                    advance(d, i, behind == 0, behind == last, options)
                else:
                    @pl.when((i >= 0) & (i < units))
                    def _():
                        advance(d, i, behind == 0, behind == last, options)

    def phase(j):
        with jax.named_scope("sharewait"):
            shared(j).wait_recv()
        if j == phases - 1:
            @pl.when(is_end)
            def _():
                for mask in range(1, n):
                    greet(mask).start()

        def step(c, carry):
            t = j * chunks + c
            if j == 0:
                load(c).wait()

                @pl.when(c + AHEAD < chunks)
                def _():
                    load(c + AHEAD).start()
            with jax.named_scope("mm"):
                part[t] = jnp.dot(g[j], v[c], preferred_element_type=jnp.float32)
            forward(t, j * chunks, (j + 1) * chunks)
            nxt = j + 1
            if nxt < phases:
                q = lax.div(c, 2)
                for h in range(2):
                    @pl.when(lax.rem(c, 2) == h)
                    def _():
                        top = top_of(nxt)
                        with jax.named_scope("shipwait"):
                            ship(h, nxt - (1 << top), nxt, q, orders[h][top]).wait_recv()
                        share(h, nxt, q).start()
                        after = nxt + 1
                        if after < phases:
                            upper = top_of(after)
                            turned = orders[1 - h][upper] == orders[h][top] and orders[h][upper] != orders[h][top]
                            k = 1 - h if turned else h
                            ship(k, after - (1 << upper), after, q, orders[k][upper]).start()
            return carry

        lax.fori_loop(0, chunks, step, 0)

    for j in range(phases):
        phase(j)

    def trail(t, carry):
        forward(t, units, units + lag)
        return carry

    lax.fori_loop(units, units + lag, trail, 0)

    row = lax.broadcasted_iota(jnp.int32, (half, LANES), 0)
    lane_of = lax.broadcasted_iota(jnp.int32, (half, LANES), 1)
    which = (mz == last).astype(jnp.int32)
    source = flipped(sum(bits))
    base = source * each + which * half
    home = lax.div(base, block)
    slot_mine = 2 * source + which
    per = block // half

    def post(step, i):
        return pltpu.make_async_remote_copy(
            src_ref=mail, dst_ref=got.at[slot_mine], send_sem=bs.at[step], recv_sem=br.at[2 - step],
            device_id={"samp": lax.rem(me + i, n), "cpg": lax.clamp(0, home + step - 1, last)}, device_id_type=MESH)

    def each_post(act):
        for step in range(3):
            plane = home + step - 1

            @pl.when((plane >= 0) & (plane <= last))
            def _():
                def body(i, carry):
                    @pl.when((i > 0) | (plane != mz))
                    def _():
                        act(post(step, i))
                    return carry

                lax.fori_loop(0, n, body, 0)

    def fold(x):
        return sum(x[:, k * LANES : (k + 1) * LANES] for k in range(CHUNK // LANES))

    def tall(x):
        return jnp.concatenate([x] * (half // 8), axis=0)

    def settle(acc):
        return [jnp.sum(x, axis=1, keepdims=True) for x in acc]

    def newton(log_scale, acc):
        crossed, energy, traced, fisher, s_r, s_p, s_q = settle(acc)
        effect = crossed / (energy + EPSILON)
        spread = s_r - 2.0 * effect * s_p + effect * effect * s_q
        gradient = 0.5 * (spread - traced)
        return log_scale + jnp.tanh(gradient / (jnp.exp(log_scale) * (0.5 * fisher)))

    @pl.when(is_end)
    def _():
        others = lamg.at[pl.ds(1, n - 1)]
        pltpu.make_async_remote_copy(
            src_ref=others, dst_ref=others, send_sem=es.at[0], recv_sem=er.at[0],
            device_id={"samp": flipped(1)}, device_id_type=MESH).wait_recv()
        acc = tuple(jnp.zeros((half if k < 5 else 8, LANES), jnp.float32) for k in range(7))
        for j in range(phases):
            for cb in range(2):
                here = j == phases - 1 and cb == 0
                slot = jnp.where(mz == 0, mask_of(0, phases - 1 - j) + cb, mask_of(1, phases - 1 - j) + cb)

                if not here:
                    pltpu.make_async_remote_copy(
                        src_ref=full.at[slot], dst_ref=full.at[slot], send_sem=hs.at[0], recv_sem=hr.at[slot],
                        device_id={"samp": flipped(1)}, device_id_type=MESH).wait_recv()

                def absorb(c, acc):
                    at = slot * chunks + c
                    a = full[slot, c, 0:half, :].astype(jnp.float32)
                    b = full[slot, c, half:pair, :].astype(jnp.float32)
                    p, q, r = a * b, b * b, a * a
                    pp[at] = p
                    qq[at] = q
                    rr[at] = r
                    lam = lamg[slot, 0:1, pl.ds(pl.multiple_of(c * CHUNK, CHUNK), CHUNK)]
                    lam = jnp.broadcast_to(lam, (8, CHUNK))
                    lb[at] = lam
                    inv = 1.0 / (lam + 1.0)
                    lev = lam * inv
                    s = tall(lev * inv)
                    inv = tall(inv)
                    terms = (p * inv, q * inv, s * r, s * p, s * q, lev, lev * lev)
                    return tuple(x + fold(y) for x, y in zip(acc, terms))

                with jax.named_scope(f"absorb{2*j+cb}"):
                    acc = lax.fori_loop(0, chunks, absorb, acc)
        crossed, energy, s_r, s_p, s_q, traced, fisher = acc
        log_scale = newton(jnp.zeros((half, 1), jnp.float32),
                           (crossed, energy, tall(traced), tall(fisher), s_r, s_p, s_q))

        def sweep(log_scale, whole):
            scale = jnp.broadcast_to(jnp.exp(log_scale), (half, CHUNK))

            def terms_of(i):
                lam = tall(lb[i])
                inv = 1.0 / (scale * lam + 1.0)
                p = pp[i] * inv
                q = qq[i] * inv
                terms = [p, q]
                if whole:
                    lev = lam * inv
                    terms += [lev, lev * lev, rr[i] * (lev * inv), p * lev, q * lev]
                return [fold(y) for y in terms]

            def body(i, acc):
                for u in range(UNROLL):
                    acc = tuple(x + y for x, y in zip(acc, terms_of(i * UNROLL + u)))
                return acc

            start = tuple(jnp.zeros((half, LANES), jnp.float32) for _ in range(7 if whole else 2))
            return lax.fori_loop(0, n * chunks // UNROLL, body, start)

        for _ in range(ITERS - 1):
            with jax.named_scope("iter"):
                log_scale = newton(log_scale, sweep(log_scale, True))
        with jax.named_scope("lastsweep"):
            crossed, energy = settle(sweep(log_scale, False))
        zscore = crossed / jnp.sqrt(energy + EPSILON)
        hit = lane_of == row + lax.rem(base, block)
        mail[0:1, :] = jnp.sum(jnp.where(hit, jnp.broadcast_to(zscore, (half, LANES)), 0.0), axis=0, keepdims=True)
        mail[1:2, :] = jnp.sum(jnp.where(hit, jnp.broadcast_to(log_scale, (half, LANES)), 0.0), axis=0, keepdims=True)
        with jax.named_scope("post"):
            each_post(lambda copy: copy.start())

        @pl.when((home >= mz - 1) & (home <= mz + 1))
        def _():
            got[slot_mine] = mail[...]

    cur = jnp.zeros((2, LANES), jnp.float32)
    before = cur
    after = cur

    def letters(k, count):
        some = got.at[pl.ds(0, count)]
        return pltpu.make_async_remote_copy(
            src_ref=some, dst_ref=some, send_sem=bs.at[k], recv_sem=br.at[k],
            device_id={"samp": flipped(1)}, device_id_type=MESH)

    for k in range(3):
        near = (mz + k - 1 >= 0) & (mz + k - 1 <= last)
        inside = is_end & (home == mz + k - 1)
        with jax.named_scope("gotwait"):
            @pl.when(near & inside)
            def _():
                letters(k, per - 1).wait_recv()

            @pl.when(near & jnp.logical_not(inside))
            def _():
                letters(k, per).wait_recv()

    for h in range(2):
        for s in range(n):
            spot = (s * each + h * half) // block
            value = got[2 * s + h]
            cur = cur + jnp.where(mz == spot, value, 0.0)
            before = before + jnp.where(mz - 1 == spot, value, 0.0)
            after = after + jnp.where(mz + 1 == spot, value, 0.0)

    def tile(x, k):
        return jnp.broadcast_to(x[k : k + 1, :], (8, LANES))

    wide = spread_out(tile(cur, 0), tile(before, 0), tile(after, 0))
    acc = jnp.zeros((8, LANES), jnp.float32)
    for o in range(2 * HALO + 1):
        shift = (HALO - o) % LANES
        near = pltpu.roll(wide, shift, 1) if shift else wide
        acc = acc + band[o] * near
    top = lax.broadcasted_iota(jnp.int32, (8, LANES), 0)
    out_ref[...] = jnp.where(top == 0, acc / band[2 * HALO + 1], tile(cur, 1))

    first = g.at[pl.ds(1, phases - 1), pl.ds(0, side)]
    pltpu.make_async_remote_copy(
        src_ref=first, dst_ref=first, send_sem=gs.at[0], recv_sem=gr.at[0, 0, 0],
        device_id={"samp": flipped(1)}, device_id_type=MESH).wait_send()
    every = g.at[:, pl.ds(0, side)]
    pltpu.make_async_remote_copy(
        src_ref=every, dst_ref=every, send_sem=ls.at[0], recv_sem=lr.at[0],
        device_id={"samp": flipped(1)}, device_id_type=MESH).wait_send()

    def passed(d):
        return pltpu.make_async_remote_copy(
            src_ref=sent.at[d], dst_ref=landed.at[d], send_sem=zs.at[d], recv_sem=zr.at[d, 0],
            device_id={"samp": flipped(1)}, device_id_type=MESH)

    @pl.when(mz < last)
    def _():
        passed(1).wait_send()

    @pl.when(mz > 0)
    def _():
        passed(0).wait_send()

    @pl.when(is_end)
    def _():
        others = lamg.at[pl.ds(1, n - 1)]
        pltpu.make_async_remote_copy(
            src_ref=others, dst_ref=others, send_sem=es.at[0], recv_sem=er.at[0],
            device_id={"samp": flipped(1)}, device_id_type=MESH).wait_send()
        handed = full.at[pl.ds(1, n - 1)]
        pltpu.make_async_remote_copy(
            src_ref=handed, dst_ref=handed, send_sem=hs.at[0], recv_sem=hr.at[0],
            device_id={"samp": flipped(1)}, device_id_type=MESH).wait_send()
        for k in range(3):
            plane = home + k - 1

            @pl.when((plane >= 0) & (plane <= last) & (plane != mz))
            def _():
                letters(k, n).wait_send()

            @pl.when(plane == mz)
            def _():
                letters(k, n - 1).wait_send()


def scores(weights, responses, phenotype, eigvecs, eigvals, positions, reaches, n, cpgs):
    each, samples = weights.shape
    comps = eigvecs.shape[1]
    chunks = comps // CHUNK
    phases = n // 2
    units = phases * chunks
    furthest = max(SKEW, (SKEW * (cpgs - 1) + 1) // 2)
    window = min(units, -(-(furthest + 1) // 8) * 8)
    half = each // 2
    pair = 2 * half
    side = 2 * pair
    total = each * n
    pieces = max(chunks // 2, 1)
    vmem = pl.BlockSpec(memory_space=pltpu.VMEM)
    hbm = pl.BlockSpec(memory_space=pl.ANY)
    dma = pltpu.SemaphoreType.DMA
    travel = pltpu.VMEM((2, units, side, CHUNK), jnp.bfloat16)
    big = pltpu.VMEM((n * chunks, half, CHUNK), jnp.float32)
    return pl.pallas_call(
        functools.partial(score_kernel, n, cpgs),
        out_shape=jax.ShapeDtypeStruct((8, LANES), jnp.float32),
        in_specs=[hbm] * 7,
        out_specs=vmem,
        scratch_shapes=[
            pltpu.VMEM((each, samples), jnp.bfloat16),
            pltpu.VMEM((each, samples), jnp.bfloat16),
            pltpu.VMEM((phases, 2 * side, samples), jnp.bfloat16),
            pltpu.VMEM((chunks, samples, CHUNK), jnp.bfloat16),
            pltpu.VMEM((units, 2 * side, CHUNK), jnp.float32),
            travel, travel,
            pltpu.VMEM((n, chunks, pair, CHUNK), jnp.bfloat16),
            big, big, big,
            pltpu.VMEM((n * chunks, 8, CHUNK), jnp.float32),
            pltpu.VMEM((n, 1, comps), jnp.float32),
            pltpu.VMEM((2, LANES), jnp.float32),
            pltpu.VMEM((2 * n, 2, LANES), jnp.float32),
            pltpu.VMEM((8, LANES), jnp.int32),
            pltpu.VMEM((2 * HALO + 2, 8, LANES), jnp.float32),
            pltpu.VMEM((1, samples), jnp.float32),
            pltpu.VMEM((1, comps), jnp.float32),
            pltpu.VMEM((1, total), jnp.int32),
            pltpu.VMEM((1, total // cpgs), jnp.int32),
            dma((6,)), dma((AHEAD,)),
            dma((1,)), dma((2, phases - 1, pieces)),
            dma((1,)), dma((phases,)),
            dma((2,)), dma((2, window)),
            dma((1,)), dma((n,)),
            dma((1,)), dma((1,)),
            dma((3,)), dma((3,)),
        ],
        compiler_params=pltpu.CompilerParams(collective_id=1, has_side_effects=True, vmem_limit_bytes=60 * 1024 * 1024),
        cost_estimate=pl.CostEstimate(flops=4 * total * samples * comps, bytes_accessed=2 * samples * comps, transcendentals=0),
        name="scores",
    )(weights, responses, phenotype[None, :], eigvecs, eigvals[None, :], positions[None, :], reaches[None, :])


def shards(responses, weights, phenotype, eigvecs, eigvals, positions, reaches):
    n, cpgs = lax.axis_size("samp"), lax.axis_size("cpg")
    out = scores(weights, responses, phenotype, eigvecs, eigvals, positions, reaches, n, cpgs)
    block = reaches.shape[0]
    return (out[0, :block], out[1, :block])


def solution(mesh):
    in_specs = (P("samp", "cpg"), P("samp", "cpg"), P("cpg"), P("cpg", "samp"), P("samp"), P(), P("cpg"))
    out_specs = (P("cpg"), P("cpg"))
    return jax.shard_map(shards, mesh=mesh, in_specs=in_specs, out_specs=out_specs, check_vma=False)
```

```python
import functools

import jax
import jax.numpy as jnp
from jax import lax
from jax.experimental import pallas as pl
from jax.experimental.pallas import tpu as pltpu
from jax.sharding import PartitionSpec as P

ITERS = 4
HALO = 8
EPSILON = 1e-06
band_width = 1000.0
MESH = pl.DeviceIdType.MESH
LANES = 128
CHUNK = 256
SKEW = 9
STRIP = 512
AHEAD = 4
GROUP = 2
UNROLL = 8


def score_kernel(n, cpgs, w_hbm, r_hbm, ph_hbm, v_hbm, lam_hbm, pos_hbm, reach_hbm, out_ref,
                 wbuf, rbuf, g, v, part, sent, landed, full, pp, qq, rr, lb, lamg, mail, got, pad, band, ph_ref, lam_ref, pos_ref, reach_ref,
                 wsem, vsem, gs, gr, ls, lr, zs, zr, hs, hr, es, er, bs, br):
    me = lax.axis_index("samp")
    mz = lax.axis_index("cpg")
    last = cpgs - 1
    each, samples = wbuf.shape
    half = each // 2
    pair = 2 * half
    side = 2 * pair
    phases = g.shape[0]
    chunks = v.shape[0]
    units = phases * chunks
    total = each * n
    block = total // cpgs
    bits = [1 << i for i in range(1, n.bit_length() - 1)]
    orders = (bits, bits[::-1])
    pieces = gr.shape[2]
    cols = samples // pieces
    is_end = (mz == 0) | (mz == last)

    def lag_of(d, k):
        turned = SKEW * k + (1 - d)
        return turned // 2 if isinstance(k, int) else lax.div(turned, 2)


    def mask_of(h, j):
        return sum(bit for i, bit in enumerate(orders[h]) if (j >> i) & 1)

    def flipped(mask):
        out = me
        bit = 1
        while bit <= mask:
            if mask & bit:
                out = out + bit - 2 * bit * lax.rem(lax.div(me, bit), 2)
            bit *= 2
        return out

    moves = ((w_hbm, wbuf), (r_hbm, rbuf), (ph_hbm, ph_ref), (pos_hbm, pos_ref), (reach_hbm, reach_ref), (lam_hbm, lam_ref))
    loads = [pltpu.make_async_copy(src, dst, wsem.at[k]) for k, (src, dst) in enumerate(moves)]
    for c in loads:
        c.start()

    def load(c):
        return pltpu.make_async_copy(v_hbm.at[:, pl.ds(pl.multiple_of(c * CHUNK, CHUNK), CHUNK)], v.at[c], vsem.at[lax.rem(c, AHEAD)])

    got[...] = jnp.zeros_like(got)
    barrier = pltpu.get_barrier_semaphore()
    for j in range(1, n):
        pl.semaphore_signal(barrier, inc=1, device_id={"samp": flipped(j)}, device_id_type=MESH)

    @pl.when(mz > 0)
    def _():
        pl.semaphore_signal(barrier, inc=1, device_id={"cpg": lax.max(mz - 1, 0)}, device_id_type=MESH)

    @pl.when(mz < last)
    def _():
        pl.semaphore_signal(barrier, inc=1, device_id={"cpg": lax.min(mz + 1, last)}, device_id_type=MESH)

    with jax.named_scope("loadwait"):
        for c in loads[:3]:
            c.wait()
    for c in range(min(AHEAD, chunks)):
        load(c).start()

    def rows_of(h, cb):
        return pl.ds(h * side + cb * pair, pair)

    def prepare(i, carry):
        at = pl.ds(pl.multiple_of(i * STRIP, STRIP), STRIP)
        root = jnp.sqrt(wbuf[:, at].astype(jnp.float32))
        weighted = (root * rbuf[:, at].astype(jnp.float32)).astype(jnp.bfloat16)
        design = (root * ph_ref[:, at]).astype(jnp.bfloat16)
        for h in range(2):
            g[0, pl.ds(h * side, half), at] = weighted[h * half : (h + 1) * half]
            g[0, pl.ds(h * side + half, half), at] = design[h * half : (h + 1) * half]
        return carry


    def piece(q):
        return pl.ds(pl.multiple_of(q * cols, cols), cols)

    def ship(h, src, dst, q, bit):
        return pltpu.make_async_remote_copy(
            src_ref=g.at[src, rows_of(h, 0), piece(q)], dst_ref=g.at[dst, rows_of(h, 0), piece(q)],
            send_sem=gs.at[0], recv_sem=gr.at[h, dst - 1, q],
            device_id={"samp": flipped(bit)}, device_id_type=MESH)

    def share(h, j, q):
        return pltpu.make_async_remote_copy(
            src_ref=g.at[j, rows_of(h, 0), piece(q)], dst_ref=g.at[j, rows_of(h, 1), piece(q)],
            send_sem=ls.at[0], recv_sem=lr.at[j],
            device_id={"samp": flipped(1)}, device_id_type=MESH)

    strips = cols // STRIP
    for q in range(pieces):
        lax.fori_loop(q * strips, (q + 1) * strips, prepare, 0)
        if q == 0:
            pl.semaphore_wait(barrier, n - 1 + (mz > 0).astype(jnp.int32) + (mz < last).astype(jnp.int32))
        for h in range(2):
            ship(h, 0, 1, q, orders[h][0]).start()
    for q in range(pieces):
        for h in range(2):
            share(h, 0, q).start()

    def shared(j):
        both = g.at[j, pl.ds(0, side)]
        return pltpu.make_async_remote_copy(
            src_ref=both, dst_ref=both, send_sem=ls.at[0], recv_sem=lr.at[j],
            device_id={"samp": flipped(1)}, device_id_type=MESH)

    def top_of(j):
        return j.bit_length() - 1

    for c in loads[3:]:
        c.wait()
    lane = lax.broadcasted_iota(jnp.int32, (8, LANES), 1)

    def spread_out(cur, before, after):
        right = pltpu.roll(after, block, 1)
        left = pltpu.roll(before, LANES - block, 1)
        return jnp.where(lane < block, cur, jnp.where(lane < block + HALO, right, left))

    def spots(b):
        at = b * block
        row = pos_ref[0:1, pl.ds(pl.multiple_of(lax.div(at, LANES) * LANES, LANES), LANES)].astype(jnp.float32)
        return pltpu.roll(jnp.broadcast_to(row, (8, LANES)), lax.rem(LANES - lax.rem(at, LANES), LANES), 1)

    pad[...] = jnp.zeros_like(pad)
    pad[0:1, 0:block] = reach_ref[...]
    reach = jnp.broadcast_to(pad[0:1, :], (8, LANES))
    places = spread_out(spots(mz), spots(lax.max(mz - 1, 0)), spots(lax.min(mz + 1, last)))
    norm = jnp.zeros((8, LANES), jnp.float32)
    for o in range(2 * HALO + 1):
        shift = (HALO - o) % LANES
        near = pltpu.roll(places, shift, 1) if shift else places
        at = mz * block + lane + (o - HALO)
        keep = (at >= 0) & (at < total) & (abs(o - HALO) <= reach)
        c = jnp.where(keep, jnp.exp(-jnp.abs(near - places) / band_width), 0.0)
        band[o] = c
        norm = norm + c
    band[2 * HALO + 1] = jnp.where(lane < block, norm, 1.0)
    lamg[0] = lam_ref[...]

    def greet(mask):
        return pltpu.make_async_remote_copy(
            src_ref=lam_ref, dst_ref=lamg.at[mask], send_sem=es.at[0], recv_sem=er.at[0],
            device_id={"samp": flipped(mask)}, device_id_type=MESH)

    def chain(d, i):
        return pltpu.make_async_remote_copy(
            src_ref=sent.at[d, i], dst_ref=landed.at[d, i], send_sem=zs.at[d], recv_sem=zr.at[d, lax.rem(i, zr.shape[1])],
            device_id={"cpg": lax.min(mz + 1, last) if d else lax.max(mz - 1, 0)}, device_id_type=MESH)

    def hand(d, j, c, cb):
        slot = mask_of(d, phases - 1 - j) | cb
        return pltpu.make_async_remote_copy(
            src_ref=sent.at[d, j * chunks + c, pl.ds(cb * pair, pair)], dst_ref=full.at[slot, c],
            send_sem=hs.at[0], recv_sem=hr.at[slot],
            device_id={"samp": flipped(slot)}, device_id_type=MESH)

    def deliver(d, i, options):
        for j in options:
            @pl.when(lax.div(i, chunks) == j)
            def _():
                c = i - j * chunks
                if j == phases - 1:
                    full[0, c] = sent[d, i, 0:pair, :]
                    hand(d, j, c, 1).start()
                elif j:
                    for held in ((0, 1) if j == 1 else (j,)):
                        for cb in range(2):
                            hand(d, held, c, cb).start()

    def advance(d, i, first, end, options):
        def own():
            return part[i, pl.ds(d * side, side), :]

        @pl.when(first)
        def _():
            sent[d, i] = own().astype(jnp.bfloat16)
            chain(d, i).start()

        @pl.when(jnp.logical_not(first))
        def _():
            chain(d, i).wait_recv()
            sent[d, i] = (own() + landed[d, i].astype(jnp.float32)).astype(jnp.bfloat16)

            @pl.when(jnp.logical_not(end))
            def _():
                chain(d, i).start()

            if options:
                @pl.when(end)
                def _():
                    deliver(d, i, options)

    lag = max(lag_of(0, last), lag_of(1, last))

    def forward(t, low, high):
        for d, behind in ((1, mz), (0, last - mz)):
            whole = lag_of(d, last)
            options = [j for j in range(phases) if low - whole < (j + 1) * chunks and high - whole > j * chunks]
            i = t - lag_of(d, behind)
            with jax.named_scope("up" if d else "down"):
                if low >= lag and high <= units:
                    advance(d, i, behind == 0, behind == last, options)
                else:
                    @pl.when((i >= 0) & (i < units))
                    def _():
                        advance(d, i, behind == 0, behind == last, options)

    def phase(j):
        with jax.named_scope("sharewait"):
            shared(j).wait_recv()
        if j == phases - 1:
            @pl.when(is_end)
            def _():
                for mask in range(1, n):
                    greet(mask).start()

        def step(c, carry):
            t = j * chunks + c
            if j == 0:
                load(c).wait()

                @pl.when(c + AHEAD < chunks)
                def _():
                    load(c + AHEAD).start()
            with jax.named_scope("mm"):
                part[t] = jnp.dot(g[j], v[c], preferred_element_type=jnp.float32)
            nxt = j + 1
            if nxt < phases:
                q = lax.div(c, 2)
                for h in range(2):
                    @pl.when(lax.rem(c, 2) == h)
                    def _():
                        top = top_of(nxt)
                        with jax.named_scope("shipwait"):
                            ship(h, nxt - (1 << top), nxt, q, orders[h][top]).wait_recv()
                        share(h, nxt, q).start()
                        after = nxt + 1
                        if after < phases:
                            upper = top_of(after)
                            turned = orders[1 - h][upper] == orders[h][top] and orders[h][upper] != orders[h][top]
                            k = 1 - h if turned else h
                            ship(k, after - (1 << upper), after, q, orders[k][upper]).start()
            forward(t, j * chunks, (j + 1) * chunks)
            return carry

        lax.fori_loop(0, chunks, step, 0)

    for j in range(phases):
        phase(j)

    def trail(t, carry):
        forward(t, units, units + lag)
        return carry

    lax.fori_loop(units, units + lag, trail, 0)

    row = lax.broadcasted_iota(jnp.int32, (half, LANES), 0)
    lane_of = lax.broadcasted_iota(jnp.int32, (half, LANES), 1)
    which = (mz == last).astype(jnp.int32)
    source = flipped(sum(bits))
    base = source * each + which * half
    home = lax.div(base, block)
    slot_mine = 2 * source + which
    per = block // half

    def post(step, i):
        return pltpu.make_async_remote_copy(
            src_ref=mail, dst_ref=got.at[slot_mine], send_sem=bs.at[step], recv_sem=br.at[2 - step],
            device_id={"samp": lax.rem(me + i, n), "cpg": lax.clamp(0, home + step - 1, last)}, device_id_type=MESH)

    def each_post(act):
        for turn_of in range(3):
            step = jnp.where(which == 0, 2 - turn_of, turn_of)
            plane = home + step - 1

            @pl.when((plane >= 0) & (plane <= last))
            def _():
                def body(i, carry):
                    @pl.when((i > 0) | (plane != mz))
                    def _():
                        act(post(step, i))
                    return carry

                lax.fori_loop(0, n, body, 0)

    def fold(x):
        return sum(x[:, k * LANES : (k + 1) * LANES] for k in range(CHUNK // LANES))

    def tall(x):
        return jnp.concatenate([x] * (half // 8), axis=0)

    def settle(acc):
        return [jnp.sum(x, axis=1, keepdims=True) for x in acc]

    def newton(log_scale, acc):
        crossed, energy, traced, fisher, s_r, s_p, s_q = settle(acc)
        effect = crossed / (energy + EPSILON)
        spread = s_r - 2.0 * effect * s_p + effect * effect * s_q
        gradient = 0.5 * (spread - traced)
        return log_scale + jnp.tanh(gradient / (jnp.exp(log_scale) * (0.5 * fisher)))

    @pl.when(is_end)
    def _():
        others = lamg.at[pl.ds(1, n - 1)]
        pltpu.make_async_remote_copy(
            src_ref=others, dst_ref=others, send_sem=es.at[0], recv_sem=er.at[0],
            device_id={"samp": flipped(1)}, device_id_type=MESH).wait_recv()
        acc = tuple(jnp.zeros((half if k < 5 else 8, LANES), jnp.float32) for k in range(7))
        for j in range(phases):
            for cb in range(2):
                here = j == phases - 1 and cb == 0
                slot = jnp.where(mz == 0, mask_of(0, phases - 1 - j) + cb, mask_of(1, phases - 1 - j) + cb)

                if not here:
                    pltpu.make_async_remote_copy(
                        src_ref=full.at[slot], dst_ref=full.at[slot], send_sem=hs.at[0], recv_sem=hr.at[slot],
                        device_id={"samp": flipped(1)}, device_id_type=MESH).wait_recv()

                def absorb(c, acc):
                    at = slot * chunks + c
                    a = full[slot, c, 0:half, :].astype(jnp.float32)
                    b = full[slot, c, half:pair, :].astype(jnp.float32)
                    p, q, r = a * b, b * b, a * a
                    pp[at] = p
                    qq[at] = q
                    rr[at] = r
                    lam = lamg[slot, 0:1, pl.ds(pl.multiple_of(c * CHUNK, CHUNK), CHUNK)]
                    lam = jnp.broadcast_to(lam, (8, CHUNK))
                    lb[at] = lam
                    inv = 1.0 / (lam + 1.0)
                    lev = lam * inv
                    s = tall(lev * inv)
                    inv = tall(inv)
                    terms = (p * inv, q * inv, s * r, s * p, s * q, lev, lev * lev)
                    return tuple(x + fold(y) for x, y in zip(acc, terms))

                with jax.named_scope(f"absorb{2*j+cb}"):
                    acc = lax.fori_loop(0, chunks // GROUP, lambda i, acc: absorb(i * GROUP + 1, absorb(i * GROUP, acc)), acc)
        crossed, energy, s_r, s_p, s_q, traced, fisher = acc
        log_scale = newton(jnp.zeros((half, 1), jnp.float32),
                           (crossed, energy, tall(traced), tall(fisher), s_r, s_p, s_q))

        def sweep(log_scale, whole):
            scale = jnp.broadcast_to(jnp.exp(log_scale), (half, CHUNK))

            def terms_of(i):
                lam = tall(lb[i])
                inv = 1.0 / (scale * lam + 1.0)
                p = pp[i] * inv
                q = qq[i] * inv
                terms = [p, q]
                if whole:
                    lev = lam * inv
                    terms += [lev, lev * lev, rr[i] * (lev * inv), p * lev, q * lev]
                return [fold(y) for y in terms]

            def body(i, acc):
                for u in range(UNROLL):
                    acc = tuple(x + y for x, y in zip(acc, terms_of(i * UNROLL + u)))
                return acc

            start = tuple(jnp.zeros((half, LANES), jnp.float32) for _ in range(7 if whole else 2))
            return lax.fori_loop(0, n * chunks // UNROLL, body, start)

        for _ in range(ITERS - 1):
            with jax.named_scope("iter"):
                log_scale = newton(log_scale, sweep(log_scale, True))
        with jax.named_scope("lastsweep"):
            crossed, energy = settle(sweep(log_scale, False))
        zscore = crossed / jnp.sqrt(energy + EPSILON)
        hit = lane_of == row + lax.rem(base, block)
        mail[0:1, :] = jnp.sum(jnp.where(hit, jnp.broadcast_to(zscore, (half, LANES)), 0.0), axis=0, keepdims=True)
        mail[1:2, :] = jnp.sum(jnp.where(hit, jnp.broadcast_to(log_scale, (half, LANES)), 0.0), axis=0, keepdims=True)
        with jax.named_scope("post"):
            each_post(lambda copy: copy.start())

        @pl.when((home >= mz - 1) & (home <= mz + 1))
        def _():
            got[slot_mine] = mail[...]

    cur = jnp.zeros((2, LANES), jnp.float32)
    before = cur
    after = cur

    def letters(k, count):
        some = got.at[pl.ds(0, count)]
        return pltpu.make_async_remote_copy(
            src_ref=some, dst_ref=some, send_sem=bs.at[k], recv_sem=br.at[k],
            device_id={"samp": flipped(1)}, device_id_type=MESH)

    for k in range(3):
        near = (mz + k - 1 >= 0) & (mz + k - 1 <= last)
        inside = is_end & (home == mz + k - 1)
        with jax.named_scope("gotwait"):
            @pl.when(near & inside)
            def _():
                letters(k, per - 1).wait_recv()

            @pl.when(near & jnp.logical_not(inside))
            def _():
                letters(k, per).wait_recv()

    for h in range(2):
        for s in range(n):
            spot = (s * each + h * half) // block
            value = got[2 * s + h]
            cur = cur + jnp.where(mz == spot, value, 0.0)
            before = before + jnp.where(mz - 1 == spot, value, 0.0)
            after = after + jnp.where(mz + 1 == spot, value, 0.0)

    def tile(x, k):
        return jnp.broadcast_to(x[k : k + 1, :], (8, LANES))

    wide = spread_out(tile(cur, 0), tile(before, 0), tile(after, 0))
    acc = jnp.zeros((8, LANES), jnp.float32)
    for o in range(2 * HALO + 1):
        shift = (HALO - o) % LANES
        near = pltpu.roll(wide, shift, 1) if shift else wide
        acc = acc + band[o] * near
    top = lax.broadcasted_iota(jnp.int32, (8, LANES), 0)
    out_ref[...] = jnp.where(top == 0, acc / band[2 * HALO + 1], tile(cur, 1))

    first = g.at[pl.ds(1, phases - 1), pl.ds(0, side)]
    pltpu.make_async_remote_copy(
        src_ref=first, dst_ref=first, send_sem=gs.at[0], recv_sem=gr.at[0, 0, 0],
        device_id={"samp": flipped(1)}, device_id_type=MESH).wait_send()
    every = g.at[:, pl.ds(0, side)]
    pltpu.make_async_remote_copy(
        src_ref=every, dst_ref=every, send_sem=ls.at[0], recv_sem=lr.at[0],
        device_id={"samp": flipped(1)}, device_id_type=MESH).wait_send()

    def passed(d):
        return pltpu.make_async_remote_copy(
            src_ref=sent.at[d], dst_ref=landed.at[d], send_sem=zs.at[d], recv_sem=zr.at[d, 0],
            device_id={"samp": flipped(1)}, device_id_type=MESH)

    @pl.when(mz < last)
    def _():
        passed(1).wait_send()

    @pl.when(mz > 0)
    def _():
        passed(0).wait_send()

    @pl.when(is_end)
    def _():
        others = lamg.at[pl.ds(1, n - 1)]
        pltpu.make_async_remote_copy(
            src_ref=others, dst_ref=others, send_sem=es.at[0], recv_sem=er.at[0],
            device_id={"samp": flipped(1)}, device_id_type=MESH).wait_send()
        handed = full.at[pl.ds(1, n - 1)]
        pltpu.make_async_remote_copy(
            src_ref=handed, dst_ref=handed, send_sem=hs.at[0], recv_sem=hr.at[0],
            device_id={"samp": flipped(1)}, device_id_type=MESH).wait_send()
        for k in range(3):
            plane = home + k - 1

            @pl.when((plane >= 0) & (plane <= last) & (plane != mz))
            def _():
                letters(k, n).wait_send()

            @pl.when(plane == mz)
            def _():
                letters(k, n - 1).wait_send()


def scores(weights, responses, phenotype, eigvecs, eigvals, positions, reaches, n, cpgs):
    each, samples = weights.shape
    comps = eigvecs.shape[1]
    chunks = comps // CHUNK
    phases = n // 2
    units = phases * chunks
    furthest = max(SKEW, (SKEW * (cpgs - 1) + 1) // 2)
    window = min(units, -(-(furthest + 1) // 8) * 8)
    half = each // 2
    pair = 2 * half
    side = 2 * pair
    total = each * n
    pieces = max(chunks // 2, 1)
    vmem = pl.BlockSpec(memory_space=pltpu.VMEM)
    hbm = pl.BlockSpec(memory_space=pl.ANY)
    dma = pltpu.SemaphoreType.DMA
    travel = pltpu.VMEM((2, units, side, CHUNK), jnp.bfloat16)
    big = pltpu.VMEM((n * chunks, half, CHUNK), jnp.float32)
    return pl.pallas_call(
        functools.partial(score_kernel, n, cpgs),
        out_shape=jax.ShapeDtypeStruct((8, LANES), jnp.float32),
        in_specs=[hbm] * 7,
        out_specs=vmem,
        scratch_shapes=[
            pltpu.VMEM((each, samples), jnp.bfloat16),
            pltpu.VMEM((each, samples), jnp.bfloat16),
            pltpu.VMEM((phases, 2 * side, samples), jnp.bfloat16),
            pltpu.VMEM((chunks, samples, CHUNK), jnp.bfloat16),
            pltpu.VMEM((units, 2 * side, CHUNK), jnp.float32),
            travel, travel,
            pltpu.VMEM((n, chunks, pair, CHUNK), jnp.bfloat16),
            big, big, big,
            pltpu.VMEM((n * chunks, 8, CHUNK), jnp.float32),
            pltpu.VMEM((n, 1, comps), jnp.float32),
            pltpu.VMEM((2, LANES), jnp.float32),
            pltpu.VMEM((2 * n, 2, LANES), jnp.float32),
            pltpu.VMEM((8, LANES), jnp.int32),
            pltpu.VMEM((2 * HALO + 2, 8, LANES), jnp.float32),
            pltpu.VMEM((1, samples), jnp.float32),
            pltpu.VMEM((1, comps), jnp.float32),
            pltpu.VMEM((1, total), jnp.int32),
            pltpu.VMEM((1, total // cpgs), jnp.int32),
            dma((6,)), dma((AHEAD,)),
            dma((1,)), dma((2, phases - 1, pieces)),
            dma((1,)), dma((phases,)),
            dma((2,)), dma((2, window)),
            dma((1,)), dma((n,)),
            dma((1,)), dma((1,)),
            dma((3,)), dma((3,)),
        ],
        compiler_params=pltpu.CompilerParams(collective_id=1, has_side_effects=True, vmem_limit_bytes=60 * 1024 * 1024),
        cost_estimate=pl.CostEstimate(flops=4 * total * samples * comps, bytes_accessed=2 * samples * comps, transcendentals=0),
        name="scores",
    )(weights, responses, phenotype[None, :], eigvecs, eigvals[None, :], positions[None, :], reaches[None, :])


def shards(responses, weights, phenotype, eigvecs, eigvals, positions, reaches):
    n, cpgs = lax.axis_size("samp"), lax.axis_size("cpg")
    out = scores(weights, responses, phenotype, eigvecs, eigvals, positions, reaches, n, cpgs)
    block = reaches.shape[0]
    return (out[0, :block], out[1, :block])


def solution(mesh):
    in_specs = (P("samp", "cpg"), P("samp", "cpg"), P("cpg"), P("cpg", "samp"), P("samp"), P(), P("cpg"))
    out_specs = (P("cpg"), P("cpg"))
    return jax.shard_map(shards, mesh=mesh, in_specs=in_specs, out_specs=out_specs, check_vma=False)
```
